128 devices in a mesh: dp: 1, vp: 128 (over z, y, x, core).
Axes of the slice: x: 4, y: 4, z: 4, core: 2. Of those that a mesh axis runs over, the one named last changes fastest.
Arguments:
- hidden: bfloat16 [4096, 1024], P(('dp', 'vp'))
- labels: int32 [4096], P(('dp', 'vp'))
- loss_weight: float32 [4096], P(('dp', 'vp'))
- norm_gain: float32 [1024], replicated
- w_unembed: bfloat16 [1024, 50432], P(None, 'vp')
Outputs:
- output 1: float32 [1], P('dp')
- output 2: bfloat16 [4096, 1024], P(('dp', 'vp'))
- output 3: float32 [1024, 50432], P('dp', 'vp')
- output 4: float32 [1024], P('dp')
All inputs are finite; a program needn't handle non-finite values.
Results may differ from the reference program's by a relative error of at most 0.001.
Values are sent between devices in bfloat16 or wider.
A program may use at most 1 GiB of HBM per device.

```python
import jax
import jax.numpy as jnp
from jax import lax

D = 1024
V = 50304
PAD_COLS = 128
TOK_DEV = 32
GROUP_SIZE = 128
VOCAB_PAD = V + PAD_COLS
TOKENS = TOK_DEV * GROUP_SIZE
LOW_IDS = V // 64
NORM_EPS = 1e-5


def setup_inputs(seed: int = 0, part: int = 0) -> dict:
    base_key = jax.random.key(seed)
    shared_key, parts_key = jax.random.split(base_key)
    part_key = jax.random.fold_in(parts_key, part)
    key_hid, key_pick, key_low, key_any, key_pad, key_wt = jax.random.split(part_key, 6)
    key_gain, key_unemb = jax.random.split(shared_key)
    hidden = jax.random.normal(key_hid, (TOKENS, D), jnp.float32).astype(jnp.bfloat16)
    tok_ids = jnp.arange(TOKENS)
    pick_low = jax.random.randint(key_pick, (TOKENS,), 0, 2)
    low_ids = jax.random.randint(key_low, (TOKENS,), 0, LOW_IDS)
    any_ids = jax.random.randint(key_any, (TOKENS,), 0, V)
    labels = jnp.where(pick_low == 0, low_ids, any_ids)
    labels = jnp.where(tok_ids == TOKENS - 1, V - 1, labels).astype(jnp.int32)
    pad_draw = jax.random.randint(key_pad, (TOKENS,), 0, 8)
    is_pad = (pad_draw == 0) & (tok_ids > 0)
    weight_val = jax.random.uniform(key_wt, (TOKENS,), jnp.float32, 0.25, 1.75)
    loss_weight = jnp.where(is_pad, 0.0, weight_val).astype(jnp.float32)
    norm_gain = 1.0 + 0.25 * jax.random.normal(key_gain, (D,), jnp.float32)
    w_unembed = (jax.random.normal(key_unemb, (D, VOCAB_PAD), jnp.float32) * (2.0 * D ** -0.5)).astype(jnp.bfloat16)
    return {"hidden": hidden, "labels": labels, "loss_weight": loss_weight, "norm_gain": norm_gain, "w_unembed": w_unembed}


def reference(hidden, labels, loss_weight, norm_gain, w_unembed):
    x_float = hidden.astype(jnp.float32)
    inv_rms = lax.rsqrt(jnp.mean(x_float * x_float, axis=-1, keepdims=True) + NORM_EPS)
    x_norm = x_float * inv_rms
    normed = (x_norm * norm_gain).astype(jnp.bfloat16)
    tok_scale = loss_weight / jnp.sum(loss_weight)
    col_ids = jnp.arange(VOCAB_PAD)[None, :]

    def block_step(d_unembed, block_in):
        normed_blk, label_blk, scale_blk = block_in
        logits = jnp.dot(normed_blk, w_unembed, preferred_element_type=jnp.float32)
        logits = jnp.where(col_ids < V, logits, -jnp.inf)
        is_target = col_ids == label_blk[:, None]
        row_max = jnp.max(logits, axis=1, keepdims=True)
        log_norm = row_max + jnp.log(jnp.sum(jnp.exp(logits - row_max), axis=1, keepdims=True))
        target = jnp.sum(jnp.where(is_target, logits, 0.0), axis=1, keepdims=True)
        tok_loss = (log_norm - target)[:, 0] * scale_blk
        d_logits = ((jnp.exp(logits - log_norm) - jnp.where(is_target, 1.0, 0.0)) * scale_blk[:, None]).astype(jnp.bfloat16)
        d_unembed = d_unembed + jnp.dot(normed_blk.T, d_logits, preferred_element_type=jnp.float32)
        d_normed = jnp.dot(d_logits, w_unembed.T, preferred_element_type=jnp.float32)
        return d_unembed, (tok_loss, d_normed)

    blocks = (normed.reshape(GROUP_SIZE, TOK_DEV, D), labels.reshape(GROUP_SIZE, TOK_DEV), tok_scale.reshape(GROUP_SIZE, TOK_DEV))
    d_unembed, (tok_loss, d_normed) = lax.scan(block_step, jnp.zeros((D, VOCAB_PAD), jnp.float32), blocks)
    d_normed = d_normed.reshape(TOKENS, D)
    mean_loss = jnp.sum(tok_loss).reshape(1)
    grad_hat = d_normed * norm_gain
    d_input = inv_rms * (grad_hat - x_norm * jnp.mean(grad_hat * x_norm, axis=-1, keepdims=True))
    d_norm_gain = jnp.sum(d_normed * x_norm, axis=0)
    return mean_loss, d_input.astype(jnp.bfloat16), d_unembed, d_norm_gain
```

```python
import functools

import jax
import jax.numpy as jnp
from jax import lax
from jax.experimental import pallas as pl
from jax.experimental.pallas import tpu as pltpu
from jax.sharding import PartitionSpec as P

NORM_EPS = 1e-5
PAD_COLS = 128
RING = 4
MESH = pl.DeviceIdType.MESH
F32 = jnp.float32
BF16 = jnp.bfloat16


def _parts(depth):
    tiles = depth // 128
    a = -(-tiles // 3)
    b = -(-(tiles - a) // 2)
    cuts = (0, a * 128, (a + b) * 128, depth)
    return tuple((cuts[i], cuts[i + 1] - cuts[i]) for i in range(3))


class _Sems:
    def __init__(self, send, recv):
        self.send, self.recv, self.used, self.open = send, recv, 0, []

    def copy(self, src, dst, device):
        k = self.used
        self.used += 1
        c = pltpu.make_async_remote_copy(
            src_ref=src, dst_ref=dst, send_sem=self.send.at[k], recv_sem=self.recv.at[k],
            device_id={"vp": device}, device_id_type=MESH)
        c.start()
        self.open.append(c)
        return c

    def drain(self):
        for c in self.open:
            c.wait_send()
        self.open = []


def _kernel(dims, hid_ref, meta_ref, gain_ref, w_ref,
            red_ref, dh_ref, dw_ref,
            acts, meta, w2, ex, dz, gp, dwp, dwrx, dwo, labc, wtc, frow, lrow,
            stat, statrx, ssum, redbuf, redrx, accbuf,
            rxa, rxb, rxc, rx2a, rx2b, rx2c, rx3,
            send_sem, recv_sem, out_sem):
    rows, depth, vloc, vpad = dims
    nblk = 512
    parts = _parts(depth)
    me = lax.axis_index("vp")
    core = lax.rem(me, 2)
    chip = me // 2
    pos = (lax.rem(chip, 4), lax.rem(chip // 4, 4), chip // 16)
    stride = (2, 8, 32)
    other = me + 1 - 2 * core

    def peer(d, step):
        q = lax.rem(pos[d] + step + 4, 4)
        return me + (q - pos[d]) * stride[d]

    def at(d, step):
        return lax.rem(pos[d] + step + 4, 4)

    def sel(**kw):
        full = {0: slice(None), 1: slice(None), 2: slice(None)}
        for k, v in kw.items():
            full[int(k[1])] = v
        return (full[2], full[1], full[0])

    def pick(pairs):
        full = {0: slice(None), 1: slice(None), 2: slice(None)}
        full.update(dict(pairs))
        return (full[2], full[1], full[0])

    sems = _Sems(send_sem, recv_sem)

    barrier = pltpu.get_barrier_semaphore()
    peers = [peer(d, s) for d in range(3) for s in (1, 2, 3)] + [other]
    for p in peers:
        pl.semaphore_signal(barrier, inc=1, device_id={"vp": p}, device_id_type=MESH)

    x = hid_ref[...].astype(F32)
    gain = gain_ref[...]
    inv = lax.rsqrt(jnp.mean(x * x, axis=-1, keepdims=True) + NORM_EPS)
    acts[pos[2], pos[1], pos[0]] = (x * inv * gain).astype(BF16)
    meta[pos[2], pos[1], pos[0]] = meta_ref[...]
    w2[core, 0:vloc, :] = w_ref[...]
    w2[core, vloc:, :] = jnp.zeros((nblk - vloc, depth), BF16)
    pl.semaphore_wait(barrier, len(peers))

    def asl(pairs, c):
        return acts.at[(*pick(pairs), slice(None), pl.ds(*c))]

    h0, h1 = slice(0, 2), slice(2, 4)
    first = []
    for r, c in enumerate(parts):
        d0 = r
        own = {0: pos[0], 1: pos[1], 2: pos[2]}
        cs = []
        for s in (1, 3, 2):
            cs.append(sems.copy(asl(own, c), asl(own, c), peer(d0, s)))
        if r == 0:
            m = meta.at[pick(own)]
            for s in (1, 3, 2):
                cs.append(sems.copy(m, m, peer(d0, s)))
        first.append(cs)
    wcopy = sems.copy(w2.at[core], w2.at[core], other)

    def ag_ring(view, d, base, hd, kind):
        src = view({**base, d: pos[d]})
        return [sems.copy(src, src, peer(d, 1)), sems.copy(src, src, peer(d, 3))]

    def ag_forward(view, d, base, hd, cs):
        cs[0].wait_recv()
        v = view({**base, d: at(d, 3), hd: h0})
        cs.append(sems.copy(v, v, peer(d, 1)))
        cs[1].wait_recv()
        v = view({**base, d: at(d, 1), hd: h1})
        cs.append(sems.copy(v, v, peer(d, 3)))

    def ag_finish(cs):
        cs[2].wait_recv()
        cs[3].wait_recv()

    def mview(pairs):
        return meta.at[pick(pairs)]

    for phase in (1, 2):
        live = []
        for r, c in enumerate(parts):
            d0, d1, d2 = r, (r + 1) % 3, (r + 2) % 3
            d = d1 if phase == 1 else d2
            base = {d2: pos[d2]} if phase == 1 else {}
            views = [functools.partial(asl, c=c)] + ([mview] if r == 0 else [])
            if phase == 1:
                for cp in first[r]:
                    cp.wait_recv()
            else:
                for item in prev[r]:
                    ag_finish(item[4])
            live.append([[v, d, base, d0, ag_ring(v, d, base, d0, None)] for v in views])
        for r in range(3):
            for v, d, base, d0, cs in live[r]:
                ag_forward(v, d, base, d0, cs)
        prev = live
    for r in range(3):
        for item in prev[r]:
            ag_finish(item[4])
    wcopy.wait_recv()

    lane = lax.broadcasted_iota(jnp.int32, (rows, 128), 1)
    row = lax.broadcasted_iota(jnp.int32, (rows, 128), 0)

    mall = meta[...].reshape(64, 128)
    lane64 = lax.broadcasted_iota(jnp.int32, (64, 128), 1)
    part_sum = jnp.sum(jnp.where((lane64 >= rows) & (lane64 < 2 * rows), mall, 0.0), axis=0, keepdims=True)
    ssum[0] = part_sum
    scopy = sems.copy(ssum.at[0], ssum.at[1], other)

    def zdot(z, _):
        a = acts[z].reshape(16 * rows, depth)
        for b in range(2):
            ex[b, z] = lax.dot_general(a, w2[b], (((1,), (1,)), ((), ())),
                                       preferred_element_type=F32).reshape(4, 4, rows, nblk)
        return 0

    lax.fori_loop(0, 4, zdot, 0)

    lane_n = lax.broadcasted_iota(jnp.int32, (rows, nblk), 1)
    bases = [(2 * chip + b) * vloc for b in range(2)]
    accbuf[...] = jnp.zeros_like(accbuf)

    def soft(i, _):
        z, y = i // 4, lax.rem(i, 4)
        mrow = jnp.zeros((1, 128), F32)
        srow = jnp.zeros((1, 128), F32)
        for xx in range(4):
            mt = jnp.broadcast_to(meta[z, y, xx], (rows, 128))
            lab = jnp.sum(jnp.where(lane == row, mt, 0.0), axis=1, keepdims=True)
            wt = jnp.sum(jnp.where(lane == row + rows, mt, 0.0), axis=1, keepdims=True)
            labc[z, y, xx] = lab
            wtc[z, y, xx] = wt
            labi = lab.astype(jnp.int32)
            vals = []
            tgt = jnp.zeros((rows, nblk), F32)
            for b in range(2):
                v = ex[b, z, y, xx]
                ok = (lane_n < vloc) & (lane_n < vpad - bases[b])
                tgt = tgt + jnp.where((lane_n == labi - bases[b]) & (lane_n < vloc), v, 0.0)
                vals.append(jnp.where(ok, v, -jnp.inf))
            mx = jnp.max(jnp.maximum(vals[0], vals[1]), axis=1, keepdims=True)
            es = [jnp.exp(v - mx) for v in vals]
            sm = jnp.sum(es[0] + es[1], axis=1, keepdims=True)
            for b in range(2):
                ex[b, z, y, xx] = es[b]
            here = lane == row + rows * xx
            mrow = mrow + jnp.sum(jnp.where(here, mx, 0.0), axis=0, keepdims=True)
            srow = srow + jnp.sum(jnp.where(here, sm, 0.0), axis=0, keepdims=True)
            accbuf[0] += tgt * wt
        stat[0, 0, z, y] = mrow
        stat[0, 1, z, y] = srow
        return 0

    lax.fori_loop(0, 16, soft, 0)

    for d in range(3):
        cs = [sems.copy(stat.at[d], statrx.at[d, s - 1], peer(d, s)) for s in (1, 2, 3)]
        ms, ss = [stat[d, 0]], [stat[d, 1]]
        for s in range(3):
            cs[s].wait_recv()
            ms.append(statrx[d, s, 0])
            ss.append(statrx[d, s, 1])
        top = functools.reduce(jnp.maximum, ms)
        tot = functools.reduce(jnp.add, [s * jnp.exp(m - top) for m, s in zip(ms, ss)])
        stat[d + 1, 0] = top
        stat[d + 1, 1] = tot
    lse = stat[3, 0] + jnp.log(stat[3, 1])
    lrow[...] = lse
    frow[...] = jnp.exp(stat[0, 0] - lse)
    scopy.wait_recv()
    total_w = jnp.sum(ssum[0] + ssum[1], axis=1, keepdims=True)

    def grad(i, _):
        z, y = i // 4, lax.rem(i, 4)
        fr = jnp.broadcast_to(frow[z, y], (rows, 128))
        lr = jnp.broadcast_to(lrow[z, y], (rows, 128))
        for xx in range(4):
            here = lane == row + rows * xx
            fc = jnp.sum(jnp.where(here, fr, 0.0), axis=1, keepdims=True)
            lab = labc[z, y, xx].astype(jnp.int32)
            sc = wtc[z, y, xx] / total_w
            accbuf[1, :, 0:128] += jnp.where(here, lr, 0.0) * sc
            for b in range(2):
                p = ex[b, z, y, xx] * fc
                hit = (lane_n == lab - bases[b]) & (lane_n < vloc)
                dz[b, z, y, xx] = ((p - jnp.where(hit, 1.0, 0.0)) * sc).astype(BF16)
        return 0

    lax.fori_loop(0, 16, grad, 0)

    def gdot(z, _):
        g = jnp.dot(dz[0, z].reshape(16 * rows, nblk), w2[0], preferred_element_type=F32)
        g = g + jnp.dot(dz[1, z].reshape(16 * rows, nblk), w2[1], preferred_element_type=F32)
        gp[z] = g.reshape(4, 4, rows, depth)
        return 0

    lax.fori_loop(0, 4, gdot, 0)

    rx1s = (rxa, rxb, rxc)
    rx2s = (rx2a, rx2b, rx2c)

    def gsl(pairs, c):
        return gp.at[(*pick(pairs), slice(None), pl.ds(*c))]

    def rs_start(bufs, c, d, hd, base):
        far = at(d, 2)
        up, dn = at(d, 1), at(d, 3)
        return [
            sems.copy(gsl({**base, d: far, hd: h0}, c), bufs.at[0], peer(d, 1)),
            sems.copy(gsl({**base, d: far, hd: h1}, c), bufs.at[1], peer(d, 3)),
            sems.copy(gsl({**base, d: up, hd: h1}, c), bufs.at[2], peer(d, 1)),
            sems.copy(gsl({**base, d: dn, hd: h0}, c), bufs.at[3], peer(d, 3)),
        ]

    def each(hd, rest, half, fixed, fn):
        if rest is None:
            for i in range(2):
                fn((i,), {**fixed, hd: 2 * half + i})
            return

        def body(t, _):
            i, j = t // 4, lax.rem(t, 4)
            idx = (i, j) if hd > rest else (j, i)
            fn(idx, {**fixed, hd: 2 * half + i, rest: j})
            return 0

        lax.fori_loop(0, 8, body, 0)

    def rs_relay(bufs, c, d, hd, rest, base, cs):
        for k, (q, half) in enumerate(((at(d, 1), 0), (at(d, 3), 1))):
            cs[k].wait_recv()

            def add(idx, pairs):
                bufs[(k, *idx)] += gp[(*pick(pairs), slice(None), pl.ds(*c))]

            each(hd, rest, half, {**base, d: q}, add)
            cs.append(sems.copy(bufs.at[k], bufs.at[4 + k], peer(d, 1 if k == 0 else 3)))

    def rs_finish(bufs, c, d, hd, rest, base, cs):
        for half, (k1, k2) in enumerate(((3, 4), (2, 5))):
            cs[k1].wait_recv()
            cs[k2].wait_recv()

            def add(idx, pairs):
                s = (*pick(pairs), slice(None), pl.ds(*c))
                gp[s] = gp[s] + (bufs[(k1, *idx)] + bufs[(k2, *idx)])

            each(hd, rest, half, {**base, d: pos[d]}, add)

    def order(r):
        return r, (r + 1) % 3, (r + 2) % 3

    cs1 = [rs_start(rx1s[r], c, order(r)[0], order(r)[1], {}) for r, c in enumerate(parts)]

    def dwdot(blk):
        dwp[blk] = jnp.zeros_like(dwp[blk])

        def body(z, _):
            dwp[blk] += lax.dot_general(dz[blk, z].reshape(16 * rows, nblk), acts[z].reshape(16 * rows, depth),
                                        (((0,), (0,)), ((), ())), preferred_element_type=F32)
            return 0

        lax.fori_loop(0, 4, body, 0)

    dwdot(1 - core)
    dwcopy = sems.copy(dwp.at[1 - core], dwrx, other)

    for r, c in enumerate(parts):
        d0, d1, d2 = order(r)
        rs_relay(rx1s[r], c, d0, d1, d2, {}, cs1[r])

    dwdot(core)
    dwcopy.wait_recv()
    dwo[...] = dwp[core, 0:vloc, :] + dwrx[0:vloc, :]
    ocopy = pltpu.make_async_copy(dwo, dw_ref, out_sem)
    ocopy.start()

    cs2 = []
    for r, c in enumerate(parts):
        d0, d1, d2 = order(r)
        rs_finish(rx1s[r], c, d0, d1, d2, {}, cs1[r])
        cs2.append(rs_start(rx2s[r], c, d1, d2, {d0: pos[d0]}))
    for r, c in enumerate(parts):
        d0, d1, d2 = order(r)
        rs_relay(rx2s[r], c, d1, d2, None, {d0: pos[d0]}, cs2[r])
    cs3 = []
    for r, c in enumerate(parts):
        d0, d1, d2 = order(r)
        base = {d0: pos[d0]}
        rs_finish(rx2s[r], c, d1, d2, None, base, cs2[r])
        base = {d0: pos[d0], d1: pos[d1]}
        cs3.append([sems.copy(gsl({**base, d2: at(d2, s)}, c), rx3.at[s - 1, :, pl.ds(*c)], peer(d2, s))
                    for s in (1, 3, 2)])
    for r in range(3):
        for cp in cs3[r]:
            cp.wait_recv()
    g = gp[pos[2], pos[1], pos[0]] + (rx3[0] + rx3[2]) + rx3[1]

    n = x * inv
    u = g * gain
    dh_ref[...] = (inv * (u - n * jnp.mean(u * n, axis=-1, keepdims=True))).astype(BF16)
    redbuf[0, 0:1, :] = jnp.sum(g * n, axis=0, keepdims=True)
    lsum = jnp.sum(accbuf[1]) * (1.0 / 64.0) - jnp.sum(accbuf[0] / total_w)
    redbuf[0, 1:2, :] = jnp.broadcast_to(lsum.reshape(1, 1), (1, depth))

    cp = sems.copy(redbuf.at[0], redrx.at[0], other)
    cp.wait_recv()
    redbuf[1] = redbuf[0] + redrx[0]
    for d in range(3):
        cs = [sems.copy(redbuf.at[1 + d], redrx.at[1 + 3 * d + s - 1], peer(d, s)) for s in (1, 2, 3)]
        for cp in cs:
            cp.wait_recv()
        tot = (redbuf[1 + d] + redrx[1 + 3 * d + 1]) + (redrx[1 + 3 * d] + redrx[1 + 3 * d + 2])
        if d < 2:
            redbuf[2 + d] = tot
        else:
            red_ref[...] = tot
    ocopy.wait()
    sems.drain()


def solution(mesh):
    def local_step(hidden, labels, loss_weight, norm_gain, w_local):
        rows, depth = hidden.shape
        vloc = w_local.shape[1]
        vpad = vloc * mesh.shape["vp"] - PAD_COLS
        meta = jnp.concatenate([labels.astype(F32), loss_weight, jnp.zeros((128 - 2 * rows,), F32)]).reshape(1, 128)
        nb = 512
        widths = [w for _, w in _parts(depth)]
        dma = pltpu.SemaphoreType.DMA
        nsem = 116
        v = pltpu.VMEM
        vm = pl.BlockSpec(memory_space=pltpu.VMEM)
        red, dh, dwt = pl.pallas_call(
            functools.partial(_kernel, (rows, depth, vloc, vpad)),
            name="head_step",
            out_shape=(jax.ShapeDtypeStruct((2, depth), F32),
                       jax.ShapeDtypeStruct((rows, depth), BF16),
                       jax.ShapeDtypeStruct((vloc, depth), F32)),
            in_specs=[vm] * 4,
            out_specs=(vm, vm, pl.BlockSpec(memory_space=pl.ANY)),
            scratch_shapes=[
                v((4, 4, 4, rows, depth), BF16),
                v((4, 4, 4, 1, 128), F32),
                v((2, nb, depth), BF16),
                v((2, 4, 4, 4, rows, nb), F32),
                v((2, 4, 4, 4, rows, nb), BF16),
                v((4, 4, 4, rows, depth), F32),
                v((2, nb, depth), F32),
                v((nb, depth), F32),
                v((vloc, depth), F32),
                v((4, 4, 4, rows, 1), F32),
                v((4, 4, 4, rows, 1), F32),
                v((4, 4, 1, 128), F32),
                v((4, 4, 1, 128), F32),
                v((4, 2, 4, 4, 1, 128), F32),
                v((3, 3, 2, 4, 4, 1, 128), F32),
                v((2, 1, 128), F32),
                v((4, 2, depth), F32),
                v((10, 2, depth), F32),
                v((2, rows, nb), F32),
                v((6, 4, 2, rows, widths[0]), F32),
                v((6, 2, 4, rows, widths[1]), F32),
                v((6, 4, 2, rows, widths[2]), F32),
                v((6, 2, rows, widths[0]), F32),
                v((6, 2, rows, widths[1]), F32),
                v((6, 2, rows, widths[2]), F32),
                v((3, rows, depth), F32),
                dma((nsem,)),
                dma((nsem,)),
                dma(()),
            ],
            compiler_params=pltpu.CompilerParams(
                collective_id=0, has_side_effects=True, vmem_limit_bytes=63 * 1024 * 1024),
        )(hidden, meta, norm_gain.reshape(1, depth), w_local.T)
        return red[1, 0:1], dh, dwt.T, red[0]

    return jax.shard_map(
        local_step,
        mesh=mesh,
        in_specs=(P(("dp", "vp"), None), P(("dp", "vp")), P(("dp", "vp")), P(None), P(None, "vp")),
        out_specs=(P("dp"), P(("dp", "vp"), None), P("dp", "vp"), P("dp")),
        check_vma=False,
    )
```

```python
import functools
import math

import jax
import jax.numpy as jnp
from jax import lax
from jax.experimental import pallas as pl
from jax.experimental.pallas import tpu as pltpu
from jax.sharding import PartitionSpec as P

NORM_EPS = 1e-5
PAD_COLS = 128
CHUNKS = 4
NBLK = 512
MESH = pl.DeviceIdType.MESH
F32 = jnp.float32
BF16 = jnp.bfloat16
AROUND = (1, 3, 2)


def _parts(depth, k):
    tiles = depth // 128
    sizes = [tiles // 3 + (1 if i < tiles % 3 else 0) for i in range(3)]
    sizes = [sizes[(i + k) % 3] for i in range(3)]
    starts = [0, sizes[0], sizes[0] + sizes[1]]
    return tuple((a * 128, n * 128) for a, n in zip(starts, sizes))


def _rowsum(x):
    return jnp.sum(x, axis=1, keepdims=True)


def _colsum(x):
    return jnp.sum(x, axis=0, keepdims=True)


def _scratch(rows, depth, vloc):
    r = rows // CHUNKS
    v = pltpu.VMEM
    c = CHUNKS
    s = {
        "xs": v((c, 4, 4, 4, r, depth), BF16),
        "acts": v((c, 4, 4, 4 * r, depth), BF16),
        "meta": v((4, 4, 4, 2, 128), F32),
        "win": v((vloc, depth), BF16),
        "w2": v((2, NBLK, depth), BF16),
        "ex": v((c, 2, 4, 4, 4, r, NBLK), F32),
        "dz": v((c, 2, 4, 4, 4 * r, NBLK), BF16),
        "gp": v((c, 4, 4, 4, r, depth), F32),
        "dwp": v((2, NBLK, depth), F32),
        "dwrx": v((NBLK, depth), F32),
        "dwo": v((vloc, depth), F32),
        "labc": v((c, 4, 4, 4 * r, 1), F32),
        "wtc": v((c, 4, 4, 4 * r, 1), F32),
        "rcol": v((c, 4, 4, 4 * r, 1), F32),
        "frow": v((c, 4, 1, 128), F32),
        "lrow": v((c, 4, 1, 128), F32),
        "stat": v((c, 4, 2, 4, 1, 128), F32),
        "statrx": v((c, 3, 3, 2, 4, 1, 128), F32),
        "ssum": v((2, 1, 128), F32),
        "dgacc": v((r, depth), F32),
        "redbuf": v((4, 2, depth), F32),
        "redrx": v((10, 2, depth), F32),
        "acct": v((4 * r, NBLK), F32),
        "accl": v((4 * r, 128), F32),
        "rx3": v((c, 3, r, depth), F32),
    }
    for k in range(c):
        for p, (_, w) in enumerate(_parts(depth, k)):
            shape = (2, 4) if p == 1 else (4, 2)
            s[f"rx1_{k}_{p}"] = v((6, *shape, r, w), F32)
            s[f"rx2_{k}_{p}"] = v((3, 4, r, w) if k == c - 1 else (6, 2, r, w), F32)
    n = 400
    s["send_sem"] = pltpu.SemaphoreType.DMA((n,))
    s["recv_sem"] = pltpu.SemaphoreType.DMA((n,))
    s["loc_sem"] = pltpu.SemaphoreType.DMA((2,))
    return s


def _pick(pairs):
    return tuple(pairs.get(d, slice(None)) for d in (2, 1, 0))


def _interleave(procs, hop=2.6, rate=46.0):
    now, link = 0.0, 0.0
    ready = [now] * len(procs)
    busy = [False] * len(procs)
    alive = set(range(len(procs)))
    while alive:
        able = [i for i in alive if ready[i] <= now]
        if able:
            i = min(able, key=lambda i: (busy[i], i))
        else:
            i = min(alive, key=lambda i: (ready[i], i))
            now = ready[i]
        try:
            step = next(procs[i])
        except StopIteration:
            alive.discard(i)
            continue
        if step is None:
            ready[i] = now + 1
            continue
        now += step[0]
        busy[i] = len(step) == 1
        ready[i] = now
        if not busy[i]:
            start = max(now, link)
            ready[i] = start + step[1] / rate + hop
            link = start + step[-1] / rate


def _kernel(dims, names, lab_ref, wt_ref, hid_ref, gain_ref, w_ref, red_ref, dh_ref, dw_ref, *refs):
    rows, depth, vloc, vreal = dims
    s = dict(zip(names, refs))
    r8 = rows // CHUNKS
    r32 = 4 * r8
    xs, acts, meta, w2, ex, dz, gp = (s[n] for n in ("xs", "acts", "meta", "w2", "ex", "dz", "gp"))
    dwp, stat, statrx, ssum = s["dwp"], s["stat"], s["statrx"], s["ssum"]
    me = lax.axis_index("vp")
    core = lax.rem(me, 2)
    chip = me // 2
    pos = (lax.rem(chip, 4), lax.rem(chip // 4, 4), chip // 16)
    stride = (2, 8, 32)
    other = me + 1 - 2 * core
    own = {0: pos[0], 1: pos[1], 2: pos[2]}
    h0, h1 = slice(0, 2), slice(2, 4)

    def at(d, step):
        return lax.rem(pos[d] + step, 4)

    def peer(d, step):
        return me + (at(d, step) - pos[d]) * stride[d]

    opened = []

    def copy(src, dst, device):
        i = len(opened)
        c = pltpu.make_async_remote_copy(
            src_ref=src, dst_ref=dst, send_sem=s["send_sem"].at[i], recv_sem=s["recv_sem"].at[i],
            device_id={"vp": device}, device_id_type=MESH)
        c.start()
        opened.append(c)
        return c

    barrier = pltpu.get_barrier_semaphore()
    peers = [peer(d, t) for d in range(3) for t in AROUND] + [other]
    for p in peers:
        pl.semaphore_signal(barrier, inc=1, device_id={"vp": p}, device_id_type=MESH)
    wload = pltpu.make_async_copy(w_ref, s["win"], s["loc_sem"].at[0])
    wload.start()

    for k in range(CHUNKS):
        xs[k, pos[2], pos[1], pos[0]] = hid_ref[k * r8:(k + 1) * r8, :]
    mine = meta.at[pos[2], pos[1], pos[0]]
    mine[...] = jnp.zeros((2, 128), F32)
    mine[0:1, 0:rows] = lab_ref[...].astype(F32)
    mine[1:2, 0:rows] = wt_ref[...]
    for n in ("dgacc", "acct", "accl"):
        s[n][...] = jnp.zeros_like(s[n])
    gain = gain_ref[...]
    pl.semaphore_wait(barrier, len(peers))

    lane = lax.broadcasted_iota(jnp.int32, (r32, 128), 1)
    row = lax.broadcasted_iota(jnp.int32, (r32, 128), 0)
    lane_n = lax.broadcasted_iota(jnp.int32, (r32, NBLK), 1)
    bases = [(2 * chip + b) * vloc for b in range(2)]
    done = {"g": 0, "dz": 0}
    shared = {}

    def mview(pairs):
        return meta.at[_pick(pairs)]

    def order(p):
        return p, (p + 1) % 3, (p + 2) % 3

    def half_mat(fn):
        lax.fori_loop(0, 2, lambda i, _: (fn(i), 0)[1], 0)

    def w_proc():
        yield 0.1,
        wload.wait()
        w2[core, 0:vloc, :] = s["win"][...]
        w2[core, vloc:, :] = jnp.zeros((NBLK - vloc, depth), BF16)
        shared["w"] = copy(w2.at[core], w2.at[core], other)
        yield 0.3,

    def chunk(k):
        parts = _parts(depth, k)
        wide = max(w for _, w in parts)
        kb = r8 * wide * 2 / 1024
        last = k == CHUNKS - 1

        def xsl(c, pairs):
            return xs.at[(k, *_pick(pairs), slice(None), pl.ds(*c))]

        def spread(view, pairs, d, src=None):
            ref = view(pairs) if src is None else src
            return [copy(ref, view(pairs), peer(d, t)) for t in AROUND]

        def views(p):
            return [functools.partial(xsl, parts[p])] + [mview] * (p + k == 0)

        def settle():
            for cp in flight:
                cp.wait_recv()
            flight.clear()

        flight = []
        for p, c in enumerate(parts):
            flight += spread(views(p)[0], own, p, hid_ref.at[pl.ds(k * r8, r8), pl.ds(*c)])
            for vw in views(p)[1:]:
                flight += spread(vw, own, p)
        yield 0.1, 2 * kb
        settle()
        for p in range(3):
            _, d, d2 = order(p)
            for vw in views(p):
                flight += spread(vw, {d: pos[d], d2: pos[d2]}, d)
        yield 0.1, 8 * kb
        settle()
        ring = []
        for p in range(3):
            d0, _, d = order(p)
            for vw in views(p):
                if k == 0:
                    flight += spread(vw, {d: pos[d]}, d)
                else:
                    src = vw({d: pos[d]})
                    ring.append((vw, d, d0, [copy(src, src, peer(d, t)) for t in (1, 3)]))
        yield (0.1, 32 * kb) if k == 0 else (0.1, 16 * kb)
        for vw, d, d0, cs in ring:
            for i, (t, h) in enumerate(((1, h0), (3, h1))):
                cs[i].wait_recv()
                vv = vw({d: at(d, 4 - t), d0: h})
                flight.append(copy(vv, vv, peer(d, t)))
        if k:
            yield 0.1, 8 * kb
        settle()

        def norm(i, _):
            z, y = i // 4, lax.rem(i, 4)
            x = xs[k, z, y].astype(F32).reshape(r32, depth)
            inv = lax.rsqrt(jnp.mean(x * x, axis=-1, keepdims=True) + NORM_EPS)
            s["rcol"][k, z, y] = inv
            acts[k, z, y] = (x * inv * gain).astype(BF16)
            return 0

        lax.fori_loop(0, 16, norm, 0)
        if k == 0:
            mall = meta[...].reshape(128, 128)
            odd = lax.rem(lax.broadcasted_iota(jnp.int32, (128, 128), 0), 2) == 1
            ssum[0] = _colsum(jnp.where(odd, mall, 0.0))
            shared["s"] = copy(ssum.at[0], ssum.at[1], other)
            shared["w"].wait_recv()
        yield 0.7,

        def zdot(i):
            a = acts[k, pl.ds(2 * i, 2)].reshape(8 * r32, depth)
            for b in range(2):
                ex[k, b, pl.ds(2 * i, 2)] = lax.dot_general(
                    a, w2[b], (((1,), (1,)), ((), ())),
                    preferred_element_type=F32).reshape(2, 4, 4, r8, NBLK)

        half_mat(zdot)
        yield 1.4,

        def soft(z, _):
            mrow = jnp.zeros((1, 128), F32)
            srow = jnp.zeros((1, 128), F32)
            for y in range(4):
                def col(j):
                    m = jnp.broadcast_to(meta[z, y, :, j:j + 1, :], (4, r8, 128)).reshape(r32, 128)
                    return _rowsum(jnp.where(lane == k * r8 + lax.rem(row, r8), m, 0.0))

                lab, wt = col(0), col(1)
                s["labc"][k, z, y] = lab
                s["wtc"][k, z, y] = wt
                labi = lab.astype(jnp.int32)
                vals = []
                tgt = jnp.zeros((r32, NBLK), F32)
                for b in range(2):
                    val = ex[k, b, z, y].reshape(r32, NBLK)
                    ok = (lane_n < vloc) & (lane_n < vreal - bases[b])
                    tgt = tgt + jnp.where((lane_n == labi - bases[b]) & (lane_n < vloc), val, 0.0)
                    vals.append(jnp.where(ok, val, -jnp.inf))
                mx = jnp.max(jnp.maximum(vals[0], vals[1]), axis=1, keepdims=True)
                es = [jnp.exp(val - mx) for val in vals]
                sm = _rowsum(es[0] + es[1])
                for b in range(2):
                    ex[k, b, z, y] = es[b].reshape(4, r8, NBLK)
                here = lane == row + r32 * y
                mrow = mrow + _colsum(jnp.where(here, mx, 0.0))
                srow = srow + _colsum(jnp.where(here, sm, 0.0))
                s["acct"][...] += tgt * wt
            stat[k, 0, 0, z] = mrow
            stat[k, 0, 1, z] = srow
            return 0

        lax.fori_loop(0, 4, soft, 0)
        cost = 1.2
        for d in range(3):
            cs = [copy(stat.at[k, d], statrx.at[k, d, i], peer(d, t)) for i, t in enumerate(AROUND)]
            yield cost, 8
            ms, ss = [stat[k, d, 0]], [stat[k, d, 1]]
            for i, cp in enumerate(cs):
                cp.wait_recv()
                ms.append(statrx[k, d, i, 0])
                ss.append(statrx[k, d, i, 1])
            top = functools.reduce(jnp.maximum, ms)
            stat[k, d + 1, 0] = top
            stat[k, d + 1, 1] = functools.reduce(jnp.add, [b * jnp.exp(a - top) for a, b in zip(ms, ss)])
            cost = 0.2
        lse = stat[k, 3, 0] + jnp.log(stat[k, 3, 1])
        s["lrow"][k] = lse
        s["frow"][k] = jnp.exp(stat[k, 0, 0] - lse)
        if k == 0:
            shared["s"].wait_recv()
        total_w = _rowsum(ssum[0] + ssum[1])

        def grad(z, _):
            for y in range(4):
                here = lane == row + r32 * y
                fr = jnp.broadcast_to(s["frow"][k, z], (r32, 128))
                lr = jnp.broadcast_to(s["lrow"][k, z], (r32, 128))
                fc = _rowsum(jnp.where(here, fr, 0.0))
                lab = s["labc"][k, z, y].astype(jnp.int32)
                sc = s["wtc"][k, z, y] / total_w
                s["accl"][...] += jnp.where(here, lr, 0.0) * sc
                for b in range(2):
                    prob = ex[k, b, z, y].reshape(r32, NBLK) * fc
                    hit = (lane_n == lab - bases[b]) & (lane_n < vloc)
                    dz[k, b, z, y] = ((prob - jnp.where(hit, 1.0, 0.0)) * sc).astype(BF16)
            return 0

        lax.fori_loop(0, 4, grad, 0)
        done["dz"] += 1

        def gdot(i):
            zz = pl.ds(2 * i, 2)
            g = jnp.dot(dz[k, 0, zz].reshape(8 * r32, NBLK), w2[0], preferred_element_type=F32)
            g = g + jnp.dot(dz[k, 1, zz].reshape(8 * r32, NBLK), w2[1], preferred_element_type=F32)
            gp[k, zz] = g.reshape(2, 4, 4, r8, depth)

        half_mat(gdot)

        def gsl(c, pairs):
            return gp.at[(k, *_pick(pairs), slice(None), pl.ds(*c))]

        def rs_start(bufs, c, d, hd, base):
            far, up, dn = at(d, 2), at(d, 1), at(d, 3)
            return [
                copy(gsl(c, {**base, d: far, hd: h0}), bufs.at[0], peer(d, 1)),
                copy(gsl(c, {**base, d: far, hd: h1}), bufs.at[1], peer(d, 3)),
                copy(gsl(c, {**base, d: up, hd: h1}), bufs.at[2], peer(d, 1)),
                copy(gsl(c, {**base, d: dn, hd: h0}), bufs.at[3], peer(d, 3)),
            ]

        def each(hd, rest, half, fixed, fn):
            if rest is None:
                for i in range(2):
                    fn((i,), {**fixed, hd: 2 * half + i})
                return

            def body(t, _):
                i, j = t // 4, lax.rem(t, 4)
                fn((i, j) if hd > rest else (j, i), {**fixed, hd: 2 * half + i, rest: j})
                return 0

            lax.fori_loop(0, 8, body, 0)

        def rs_relay(bufs, c, d, hd, rest, base, cs):
            for i, (q, half) in enumerate(((at(d, 1), 0), (at(d, 3), 1))):
                cs[i].wait_recv()

                def add(idx, pairs):
                    bufs[(i, *idx)] += gp[(k, *_pick(pairs), slice(None), pl.ds(*c))]

                each(hd, rest, half, {**base, d: q}, add)
                cs.append(copy(bufs.at[i], bufs.at[4 + i], peer(d, 1 if i == 0 else 3)))

        def rs_finish(bufs, c, d, hd, rest, base, cs):
            for half, (k1, k2) in enumerate(((3, 4), (2, 5))):
                cs[k1].wait_recv()
                cs[k2].wait_recv()

                def add(idx, pairs):
                    sl = (k, *_pick(pairs), slice(None), pl.ds(*c))
                    gp[sl] = gp[sl] + (bufs[(k1, *idx)] + bufs[(k2, *idx)])

                each(hd, rest, half, {**base, d: pos[d]}, add)

        rx1 = [s[f"rx1_{k}_{p}"] for p in range(3)]
        rx2 = [s[f"rx2_{k}_{p}"] for p in range(3)]
        cs1 = [rs_start(rx1[p], c, order(p)[0], order(p)[1], {}) for p, c in enumerate(parts)]
        yield 2.2, 16 * kb, 32 * kb

        def dg(i, _):
            z, y = i // 4, lax.rem(i, 4)
            n = xs[k, z, y].astype(F32).reshape(r32, depth) * s["rcol"][k, z, y]
            t = gp[k, z, y].reshape(r32, depth) * n
            s["dgacc"][...] += jnp.sum(t.reshape(4, r8, depth), axis=0)
            return 0

        lax.fori_loop(0, 16, dg, 0)
        done["g"] += 1
        for p, c in enumerate(parts):
            d0, d1, d2 = order(p)
            rs_relay(rx1[p], c, d0, d1, d2, {}, cs1[p])
        yield 0.7, 16 * kb
        cs2 = []
        for p, c in enumerate(parts):
            d0, d1, d2 = order(p)
            rs_finish(rx1[p], c, d0, d1, d2, {}, cs1[p])
            base = {d0: pos[d0]}
            if last:
                cs2.append([copy(gsl(c, {**base, d1: at(d1, t)}), rx2[p].at[i], peer(d1, t))
                            for i, t in enumerate(AROUND)])
            else:
                cs2.append(rs_start(rx2[p], c, d1, d2, base))
        yield (0.4, 16 * kb) if last else (0.4, 4 * kb, 8 * kb)
        if not last:
            for p, c in enumerate(parts):
                d0, d1, d2 = order(p)
                rs_relay(rx2[p], c, d1, d2, None, {d0: pos[d0]}, cs2[p])
            yield 0.2, 4 * kb
        cs3 = []
        for p, c in enumerate(parts):
            d0, d1, d2 = order(p)
            base = {d0: pos[d0], d1: pos[d1]}
            if last:
                for cp in cs2[p]:
                    cp.wait_recv()
                for j in range(4):
                    sl = (k, *_pick({**base, d2: j}), slice(None), pl.ds(*c))
                    gp[sl] = (gp[sl] + rx2[p][2, j]) + (rx2[p][0, j] + rx2[p][1, j])
            else:
                rs_finish(rx2[p], c, d1, d2, None, {d0: pos[d0]}, cs2[p])
            cs3 += [copy(gsl(c, {**base, d2: at(d2, t)}), s["rx3"].at[k, i, :, pl.ds(*c)], peer(d2, t))
                    for i, t in enumerate(AROUND)]
        yield 0.2, 4 * kb
        for cp in cs3:
            cp.wait_recv()
        g = gp[k, pos[2], pos[1], pos[0]] + (s["rx3"][k, 0] + s["rx3"][k, 1]) + s["rx3"][k, 2]
        x = hid_ref[k * r8:(k + 1) * r8, :].astype(F32)
        inv = lax.rsqrt(jnp.mean(x * x, axis=-1, keepdims=True) + NORM_EPS)
        n = x * inv
        u = g * gain
        dh_ref[k * r8:(k + 1) * r8, :] = (inv * (u - n * jnp.mean(u * n, axis=-1, keepdims=True))).astype(BF16)
        yield 0.3,

    def dw_proc():
        while done["dz"] < CHUNKS:
            yield None
        for first in (True, False):
            blk = 1 - core if first else core
            for k in range(CHUNKS):
                def part():
                    return lax.dot_general(dz[k, blk].reshape(16 * r32, NBLK), acts[k].reshape(16 * r32, depth),
                                           (((0,), (0,)), ((), ())), preferred_element_type=F32)

                if k == 0:
                    dwp[blk] = part()
                else:
                    dwp[blk] += part()
                if k < CHUNKS - 1:
                    yield 0.8,
            if first:
                cp = copy(dwp.at[blk], s["dwrx"], other)
            yield 0.8,
        cp.wait_recv()
        s["dwo"][...] = dwp[core, 0:vloc, :] + s["dwrx"][0:vloc, :]
        shared["o"] = pltpu.make_async_copy(s["dwo"], dw_ref, s["loc_sem"].at[1])
        shared["o"].start()
        yield 0.5,

    def red_proc():
        while done["g"] < CHUNKS:
            yield None
        redbuf, redrx = s["redbuf"], s["redrx"]
        total_w = _rowsum(ssum[0] + ssum[1])
        redbuf[0, 0:1, :] = _colsum(s["dgacc"][...])
        lsum = jnp.sum(s["accl"][...]) * (1.0 / 64.0) - jnp.sum(s["acct"][...] / total_w)
        redbuf[0, 1:2, :] = jnp.broadcast_to(lsum.reshape(1, 1), (1, depth))
        cp = copy(redbuf.at[0], redrx.at[0], other)
        yield 0.3, 1
        cp.wait_recv()
        redbuf[1] = redbuf[0] + redrx[0]
        for d in range(3):
            cs = [copy(redbuf.at[1 + d], redrx.at[1 + 3 * d + i], peer(d, t)) for i, t in enumerate(AROUND)]
            yield 0.1, 24
            for cp in cs:
                cp.wait_recv()
            tot = redbuf[1 + d] + jnp.sum(redrx[pl.ds(1 + 3 * d, 3)], axis=0)
            if d < 2:
                redbuf[2 + d] = tot
            else:
                red_ref[...] = tot

    _interleave([chunk(k) for k in range(CHUNKS)] + [w_proc(), red_proc(), dw_proc()])
    shared["o"].wait()
    for c in opened:
        c.wait_send()


def _finish(red_ref, dh_ref, dw_ref, loss_out, dh_out, dw_out, dg_out, buf, sem):
    get = pltpu.make_async_copy(dw_ref, buf, sem.at[0])
    get.start()
    loss_out[...] = red_ref[1:2, 0:1]
    dg_out[...] = red_ref[0:1, :]
    dh_out[...] = dh_ref[...]
    get.wait()
    put = pltpu.make_async_copy(buf, dw_out, sem.at[1])
    put.start()
    put.wait()


def solution(mesh):
    def local_step(hidden, labels, loss_weight, norm_gain, w_local):
        rows, depth = hidden.shape
        vloc = w_local.shape[1]
        vreal = vloc * mesh.shape["vp"] - PAD_COLS
        vm = pl.BlockSpec(memory_space=pltpu.VMEM)
        hbm = pl.BlockSpec(memory_space=pl.ANY)
        scratch = _scratch(rows, depth, vloc)
        red, dh, dwt = pl.pallas_call(
            functools.partial(_kernel, (rows, depth, vloc, vreal), tuple(scratch)),
            name="head_step",
            out_shape=(jax.ShapeDtypeStruct((2, depth), F32),
                       jax.ShapeDtypeStruct((rows, depth), BF16),
                       jax.ShapeDtypeStruct((vloc, depth), F32)),
            in_specs=[vm, vm, vm, vm, hbm],
            out_specs=(vm, vm, hbm),
            scratch_shapes=list(scratch.values()),
            compiler_params=pltpu.CompilerParams(
                collective_id=0, has_side_effects=True, vmem_limit_bytes=63 * 1024 * 1024),
        )(labels.reshape(1, rows), loss_weight.reshape(1, rows), hidden, norm_gain.reshape(1, depth), w_local.T)
        loss, dh, dwt, dg = pl.pallas_call(
            _finish,
            name="head_out",
            out_shape=(jax.ShapeDtypeStruct((1, 1), F32),
                       jax.ShapeDtypeStruct((rows, depth), BF16),
                       jax.ShapeDtypeStruct((vloc, depth), F32),
                       jax.ShapeDtypeStruct((1, depth), F32)),
            in_specs=[vm, vm, hbm],
            out_specs=(vm, vm, hbm, vm),
            scratch_shapes=[pltpu.VMEM((vloc, depth), F32), pltpu.SemaphoreType.DMA((2,))],
        )(red, dh, dwt)
        return loss.reshape(1), dh, dwt.T, dg.reshape(depth)

    return jax.shard_map(
        local_step,
        mesh=mesh,
        in_specs=(P(("dp", "vp"), None), P(("dp", "vp")), P(("dp", "vp")), P(None), P(None, "vp")),
        out_specs=(P("dp"), P(("dp", "vp"), None), P("dp", "vp"), P("dp")),
        check_vma=False,
    )
```

```python
import functools
import math
import math

import jax
import jax.numpy as jnp
from jax import lax
from jax.experimental import pallas as pl
from jax.experimental.pallas import tpu as pltpu
from jax.sharding import PartitionSpec as P

NORM_EPS = 1e-5
PAD_COLS = 128
CHUNKS = 4
NBLK = 512
MESH = pl.DeviceIdType.MESH
F32 = jnp.float32
BF16 = jnp.bfloat16
AROUND = (1, 3, 2)
ORDER = (
    "22314430123012012300102232110133230123012361666003626211",
    "6603536215201321052130",
)
UNIT = 16384


def _around(*dims):
    offs = [{}]
    for d in dims:
        offs = [{**o, d: t} for t in (*AROUND, 0) for o in offs]
    return [o for o in offs if any(o.values())]


def _parts(depth, k):
    tiles = depth // 128
    sizes = [tiles // 3 + (1 if i < tiles % 3 else 0) for i in range(3)]
    sizes = [sizes[(i + k) % 3] for i in range(3)]
    starts = [0, sizes[0], sizes[0] + sizes[1]]
    return tuple((a * 128, n * 128) for a, n in zip(starts, sizes))


def _rowsum(x):
    return jnp.sum(x, axis=1, keepdims=True)


def _colsum(x):
    return jnp.sum(x, axis=0, keepdims=True)


def _scratch(rows, depth, vloc):
    r = rows // CHUNKS
    v = pltpu.VMEM
    c = CHUNKS
    s = {
        "xs": v((c, 4, 4, 4, r, depth), BF16),
        "acts": v((c, 4, 4, 4 * r, depth), BF16),
        "meta": v((4, 4, 4, 2, 128), F32),
        "win": v((vloc, depth), BF16),
        "w2": v((2, NBLK, depth), BF16),
        "ex": v((c, 2, 4, 4, 4, r, NBLK), F32),
        "dz": v((c, 2, 4, 4, 4 * r, NBLK), BF16),
        "gp": v((c, 4, 4, 4, r, depth), F32),
        "dwp": v((2, NBLK, depth), F32),
        "dwrx": v((NBLK, depth), F32),
        "dwo": v((vloc, depth), F32),
        "labc": v((c, 4, 4, 4 * r, 1), F32),
        "wtc": v((c, 4, 4, 4 * r, 1), F32),
        "rcol": v((c, 4, 4, 4 * r, 1), F32),
        "frow": v((c, 4, 1, 128), F32),
        "lrow": v((c, 4, 1, 128), F32),
        "stat": v((c, 3, 4, 1, 128), F32),
        "mloc": v((c, 4, 1, 128), F32),
        "statrx": v((c, 18, 4, 1, 128), F32),
        "ssum": v((2, 2, 128), F32),
        "dgacc": v((r, depth), F32),
        "redbuf": v((4, 1, depth + 256), F32),
        "redrx": v((19, 1, depth + 256), F32),
        "acct": v((4 * r, NBLK), F32),
        "accl": v((4 * r, 128), F32),
        "rx3": v((c, 3, r, depth), F32),
        "dum": v((64, UNIT // 2 // depth, depth), BF16),
        "dum1": v((128, 2, 128), F32),
        "hidv": v((rows, depth), BF16),
        "labv": v((1, rows), jnp.int32),
        "wtv": v((1, rows), F32),
        "gainv": v((1, depth), F32),
    }
    for k in range(c):
        for p, (_, w) in enumerate(_parts(depth, k)):
            shape = (2, 4) if p == 1 else (4, 2)
            s[f"rx1_{k}_{p}"] = v((6, *shape, r, w), F32)
            s[f"rx2_{k}_{p}"] = v((15, r, w) if k == c - 1 else (6, 2, r, w), F32)
    n = 96
    s["send_sem"] = pltpu.SemaphoreType.DMA((n,))
    s["recv_sem"] = pltpu.SemaphoreType.DMA((n,))
    s["loc_sem"] = pltpu.SemaphoreType.DMA((6,))
    return s


def _pick(pairs):
    return tuple(pairs.get(d, slice(None)) for d in (2, 1, 0))


def _interleave(procs):
    for i in map(int, "".join(ORDER)):
        next(procs[i], None)
    for p in procs:
        next(p, None)


def _kernel(dims, names, lab_ref, wt_ref, hid_in, gain_in, w_ref, red_ref, dh_ref, dw_ref, *refs):
    rows, depth, vloc, vreal = dims
    s = dict(zip(names, refs))
    r8 = rows // CHUNKS
    r32 = 4 * r8
    xs, acts, meta, w2, ex, dz, gp = (s[n] for n in ("xs", "acts", "meta", "w2", "ex", "dz", "gp"))
    dwp, stat, statrx, ssum = s["dwp"], s["stat"], s["statrx"], s["ssum"]
    me = lax.axis_index("vp")
    core = lax.rem(me, 2)
    chip = me // 2
    pos = (lax.rem(chip, 4), lax.rem(chip // 4, 4), chip // 16)
    stride = (2, 8, 32)
    other = me + 1 - 2 * core
    own = {0: pos[0], 1: pos[1], 2: pos[2]}
    h0, h1 = slice(0, 2), slice(2, 4)

    def at(d, step):
        return lax.rem(pos[d] + step, 4)

    def peer(off):
        return me + sum((at(d, t) - pos[d]) * stride[d] for d, t in off.items())

    groups = []

    class Group:
        def __init__(self):
            self.sems = s["send_sem"].at[len(groups)], s["recv_sem"].at[len(groups)]
            self.size, self.copies, self.got, self.sent = 0, [], False, False
            groups.append(self)

        def add(self, src, dst, device):
            c = pltpu.make_async_remote_copy(
                src_ref=src, dst_ref=dst, send_sem=self.sems[0], recv_sem=self.sems[1],
                device_id={"vp": device}, device_id_type=MESH)
            c.start()
            self.size += math.prod(src.shape) * src.dtype.itemsize
            self.copies.append(c)
            return self

        def _all(self, sem):
            ref = s["dum"] if self.size % UNIT == 0 else s["dum1"]
            unit = math.prod(ref.shape[1:]) * ref.dtype.itemsize
            part = ref.at[pl.ds(0, self.size // unit)]
            return pltpu.make_async_copy(part, part, sem)

        def wait_recv(self):
            self.got = True
            if len(self.copies) == 1:
                self.copies[0].wait_recv()
            else:
                self._all(self.sems[1]).wait()

        def wait_send(self):
            if self.sent:
                return
            self.sent = True
            if len(self.copies) == 1:
                self.copies[0].wait_send()
            else:
                self._all(self.sems[0]).wait()

    def copy(src, dst, device):
        return Group().add(src, dst, device)

    barrier = pltpu.get_barrier_semaphore()
    peers = [peer(o) for d in range(3) for o in _around(d)] + [other]
    for p in peers:
        pl.semaphore_signal(barrier, inc=1, device_id={"vp": p}, device_id_type=MESH)
    hid_ref, lab_v, wt_v, gain_v = (s[n] for n in ("hidv", "labv", "wtv", "gainv"))
    loads = [pltpu.make_async_copy(a, b, s["loc_sem"].at[i]) for i, (a, b) in enumerate(
        ((hid_in, hid_ref), (lab_ref, lab_v), (wt_ref, wt_v), (gain_in, gain_v), (w_ref, s["win"])))]
    for c in loads:
        c.start()
    wload = loads.pop()
    for n in ("dgacc", "acct", "accl"):
        s[n][...] = jnp.zeros_like(s[n])
    for c in loads:
        c.wait()

    for k in range(CHUNKS):
        xs[k, pos[2], pos[1], pos[0]] = hid_ref[k * r8:(k + 1) * r8, :]
    mine = meta.at[pos[2], pos[1], pos[0]]
    mine[...] = jnp.zeros((2, 128), F32)
    mine[0:1, 0:rows] = lab_v[...].astype(F32)
    mine[1:2, 0:rows] = wt_v[...]
    gain = gain_v[...]
    pl.semaphore_wait(barrier, len(peers))

    lane = lax.broadcasted_iota(jnp.int32, (r32, 128), 1)
    row = lax.broadcasted_iota(jnp.int32, (r32, 128), 0)
    lane_n = lax.broadcasted_iota(jnp.int32, (r32, NBLK), 1)
    bases = [(2 * chip + b) * vloc for b in range(2)]
    shared = {}

    def mview(pairs):
        return meta.at[_pick(pairs)]

    def order(p):
        return p, (p + 1) % 3, (p + 2) % 3

    def half_mat(fn):
        lax.fori_loop(0, 2, lambda i, _: (fn(i), 0)[1], 0)

    def w_proc():
        yield
        wload.wait()
        w2[core, 0:vloc, :] = s["win"][...]
        w2[core, vloc:, :] = jnp.zeros((NBLK - vloc, depth), BF16)
        shared["w"] = copy(w2.at[core], w2.at[core], other)
        yield

    def chunk(k):
        parts = _parts(depth, k)
        last = k == CHUNKS - 1

        def xsl(c, pairs):
            return xs.at[(k, *_pick(pairs), slice(None), pl.ds(*c))]

        def spread(group, view, pairs, dims, src=None):
            ref = view(pairs) if src is None else src
            for o in _around(*dims):
                group.add(ref, view(pairs), peer(o))

        def views(p):
            return [functools.partial(xsl, parts[p])] + [mview] * (p + k == 0)

        def fresh():
            flight[:] = [Group() for _ in range(1 if k else 2)]
            return flight

        def settle():
            for cp in flight:
                cp.wait_recv()

        flight = []
        if k:
            yield
        fresh()
        for p, c in enumerate(parts):
            dims = order(p)[:1]
            spread(flight[0], views(p)[0], own, dims, hid_ref.at[pl.ds(k * r8, r8), pl.ds(*c)])
            for vw in views(p)[1:]:
                spread(flight[1], vw, own, dims)
        yield
        settle()
        fresh()
        for p in range(3):
            _, d, d2 = order(p)
            for i, vw in enumerate(views(p)):
                spread(flight[i], vw, {d: pos[d], d2: pos[d2]}, (d,))
        yield
        settle()
        if k:
            ring = [Group(), Group()]
        else:
            fresh()
        for p in range(3):
            _, _, d = order(p)
            for i, vw in enumerate(views(p)):
                if k == 0:
                    spread(flight[i], vw, {d: pos[d]}, (d,))
                else:
                    src = vw({d: pos[d]})
                    for g, t in zip(ring, (1, 3)):
                        g.add(src, src, peer({d: t}))
        yield
        if k:
            fresh()
            for g, t, h in zip(ring, (1, 3), (h0, h1)):
                g.wait_recv()
                for p, c in enumerate(parts):
                    d0, _, d = order(p)
                    vv = xsl(c, {d: at(d, 4 - t), d0: h})
                    flight[0].add(vv, vv, peer({d: t}))
        if k:
            yield
        settle()

        def norm(z, _):
            for y in range(4):
                x = xs[k, z, y].astype(F32).reshape(r32, depth)
                inv = lax.rsqrt(jnp.mean(x * x, axis=-1, keepdims=True) + NORM_EPS)
                s["rcol"][k, z, y] = inv
                acts[k, z, y] = (x * inv * gain).astype(BF16)
            return 0

        lax.fori_loop(0, 4, norm, 0)
        if k == 0:
            ssum[0] = jnp.sum(meta[...].reshape(64, 2, 128), axis=0)
            shared["s"] = copy(ssum.at[0], ssum.at[1], other)
            shared["w"].wait_recv()
        yield

        def zdot(i):
            a = acts[k, pl.ds(2 * i, 2)].reshape(8 * r32, depth)
            for b in range(2):
                ex[k, b, pl.ds(2 * i, 2)] = lax.dot_general(
                    a, w2[b], (((1,), (1,)), ((), ())),
                    preferred_element_type=F32).reshape(2, 4, 4, r8, NBLK)

        half_mat(zdot)
        yield

        def soft(z, _):
            mrow = jnp.zeros((1, 128), F32)
            srow = jnp.zeros((1, 128), F32)
            for y in range(4):
                def col(j):
                    m = jnp.broadcast_to(meta[z, y, :, j:j + 1, :], (4, r8, 128)).reshape(r32, 128)
                    return _rowsum(jnp.where(lane == k * r8 + lax.rem(row, r8), m, 0.0))

                lab, wt = col(0), col(1)
                s["labc"][k, z, y] = lab
                s["wtc"][k, z, y] = wt
                labi = lab.astype(jnp.int32)
                vals = []
                tgt = jnp.zeros((r32, NBLK), F32)
                for b in range(2):
                    val = ex[k, b, z, y].reshape(r32, NBLK)
                    ok = (lane_n < vloc) & (lane_n < vreal - bases[b])
                    tgt = tgt + jnp.where((lane_n == labi - bases[b]) & (lane_n < vloc), val, 0.0)
                    vals.append(jnp.where(ok, val, -jnp.inf))
                mx = jnp.max(jnp.maximum(vals[0], vals[1]), axis=1, keepdims=True)
                es = [jnp.exp(val - mx) for val in vals]
                sm = _rowsum(es[0] + es[1])
                for b in range(2):
                    ex[k, b, z, y] = es[b].reshape(4, r8, NBLK)
                here = lane == row + r32 * y
                mrow = mrow + _colsum(jnp.where(here, mx, 0.0))
                srow = srow + _colsum(jnp.where(here, sm, 0.0))
                s["acct"][...] += tgt * wt
            s["mloc"][k, z] = mrow
            stat[k, 0, z] = mrow + jnp.log(srow)
            return 0

        lax.fori_loop(0, 4, soft, 0)
        for i, dims in enumerate(((0, 1), (2,))):
            offs = _around(*dims)
            rx = statrx.at[k, pl.ds(15 * i, len(offs))]
            g = Group()
            for j, o in enumerate(offs):
                g.add(stat.at[k, i], rx.at[j], peer(o))
            yield
            g.wait_recv()
            mine = stat[k, i]
            got = rx[...]
            top = jnp.maximum(mine, jnp.max(got, axis=0))
            stat[k, i + 1] = top + jnp.log(jnp.exp(mine - top) + jnp.sum(jnp.exp(got - top), axis=0))
        lse = stat[k, 2]
        s["lrow"][k] = lse
        s["frow"][k] = jnp.exp(s["mloc"][k] - lse)
        if k == 0:
            shared["s"].wait_recv()
        total_w = _rowsum(ssum[0, 1:] + ssum[1, 1:])

        def grad(z, _):
            for y in range(4):
                here = lane == row + r32 * y
                fr = jnp.broadcast_to(s["frow"][k, z], (r32, 128))
                lr = jnp.broadcast_to(s["lrow"][k, z], (r32, 128))
                fc = _rowsum(jnp.where(here, fr, 0.0))
                lab = s["labc"][k, z, y].astype(jnp.int32)
                sc = s["wtc"][k, z, y] / total_w
                s["accl"][...] += jnp.where(here, lr, 0.0) * sc
                for b in range(2):
                    prob = ex[k, b, z, y].reshape(r32, NBLK) * fc
                    hit = (lane_n == lab - bases[b]) & (lane_n < vloc)
                    dz[k, b, z, y] = ((prob - jnp.where(hit, 1.0, 0.0)) * sc).astype(BF16)
            return 0

        lax.fori_loop(0, 4, grad, 0)

        def gdot(i):
            zz = pl.ds(2 * i, 2)
            g = jnp.dot(dz[k, 0, zz].reshape(8 * r32, NBLK), w2[0], preferred_element_type=F32)
            g = g + jnp.dot(dz[k, 1, zz].reshape(8 * r32, NBLK), w2[1], preferred_element_type=F32)
            gp[k, zz] = g.reshape(2, 4, 4, r8, depth)

        half_mat(gdot)

        def gsl(c, pairs):
            return gp.at[(k, *_pick(pairs), slice(None), pl.ds(*c))]

        def rs_far(bufs, c, d, hd, base, gs):
            for i, (g, h, t) in enumerate(zip(gs, (h0, h1), (1, 3))):
                g.add(gsl(c, {**base, d: at(d, 2), hd: h}), bufs.at[i], peer({d: t}))

        def rs_near(bufs, c, d, hd, base, gs):
            for i, (h, t) in enumerate(zip((h1, h0), (1, 3))):
                gs[2].add(gsl(c, {**base, d: at(d, t), hd: h}), bufs.at[2 + i], peer({d: t}))

        def triple():
            return [Group() for _ in range(3)]

        def each(hd, rest, half, fixed, fn):
            if rest is None:
                for i in range(2):
                    fn((i,), {**fixed, hd: 2 * half + i})
                return

            def body(t, _):
                i, j = t // 4, lax.rem(t, 4)
                fn((i, j) if hd > rest else (j, i), {**fixed, hd: 2 * half + i, rest: j})
                return 0

            lax.fori_loop(0, 8, body, 0)

        def rs_relay(todo, gs):
            for i, t in enumerate((1, 3)):
                gs[i].wait_recv()
                for bufs, c, d, hd, rest, base in todo:
                    def add(idx, pairs):
                        bufs[(i, *idx)] += gp[(k, *_pick(pairs), slice(None), pl.ds(*c))]

                    each(hd, rest, i, {**base, d: at(d, t)}, add)
                    gs[2].add(bufs.at[i], bufs.at[4 + i], peer({d: t}))

        def rs_finish(bufs, c, d, hd, rest, base):
            for half, (k1, k2) in enumerate(((3, 4), (2, 5))):
                def add(idx, pairs):
                    sl = (k, *_pick(pairs), slice(None), pl.ds(*c))
                    gp[sl] = gp[sl] + (bufs[(k1, *idx)] + bufs[(k2, *idx)])

                each(hd, rest, half, {**base, d: pos[d]}, add)

        rx1 = [s[f"rx1_{k}_{p}"] for p in range(3)]
        rx2 = [s[f"rx2_{k}_{p}"] for p in range(3)]
        todo1 = [(rx1[p], c, *order(p), {}) for p, c in enumerate(parts)]
        todo2 = [(rx2[p], c, order(p)[1], order(p)[2], None, {p: pos[p]}) for p, c in enumerate(parts)]
        gs1 = triple()
        for bufs, c, d, hd, _, base in todo1:
            rs_far(bufs, c, d, hd, base, gs1)
        yield
        for bufs, c, d, hd, _, base in todo1:
            rs_near(bufs, c, d, hd, base, gs1)
        yield

        def dg(z, _):
            acc = jnp.zeros((r8, depth), F32)
            for y in range(4):
                n = xs[k, z, y].astype(F32).reshape(r32, depth) * s["rcol"][k, z, y]
                t = gp[k, z, y].reshape(r32, depth) * n
                acc = acc + jnp.sum(t.reshape(4, r8, depth), axis=0)
            s["dgacc"][...] += acc
            return 0

        lax.fori_loop(0, 4, dg, 0)
        yield
        rs_relay(todo1, gs1)
        yield
        gs1[2].wait_recv()
        gs2 = [Group()] if last else triple()
        for t1, (bufs, c, d, hd, _, base) in zip(todo1, todo2):
            rs_finish(*t1)
            if last:
                for i, o in enumerate(_around(d, hd)):
                    gs2[0].add(gsl(c, {**base, **{e: at(e, o[e]) for e in o}}), bufs.at[i], peer(o))
            else:
                rs_far(bufs, c, d, hd, base, gs2)
                rs_near(bufs, c, d, hd, base, gs2)
        yield
        if last:
            for g in groups:
                if g.got:
                    g.wait_send()
            gs2[0].wait_recv()
            for bufs, c, *_ in todo2:
                s["rx3"][k, 0, :, pl.ds(*c)] = jnp.sum(bufs[...], axis=0)
        else:
            rs_relay(todo2, gs2)
            yield
            gs2[2].wait_recv()
            g3 = Group()
            for t2 in todo2:
                rs_finish(*t2)
                _, c, d1, d, _, base = t2
                for i, t in enumerate(AROUND):
                    g3.add(gsl(c, {**base, d1: pos[d1], d: at(d, t)}), s["rx3"].at[k, i, :, pl.ds(*c)], peer({d: t}))
            yield
            g3.wait_recv()
        g = gp[k, pos[2], pos[1], pos[0]]
        for i in range(1 if last else 3):
            g = g + s["rx3"][k, i]
        x = hid_ref[k * r8:(k + 1) * r8, :].astype(F32)
        inv = lax.rsqrt(jnp.mean(x * x, axis=-1, keepdims=True) + NORM_EPS)
        n = x * inv
        u = g * gain
        dh_ref[k * r8:(k + 1) * r8, :] = (inv * (u - n * jnp.mean(u * n, axis=-1, keepdims=True))).astype(BF16)
        yield

    def dw_proc():
        for first in (True, False):
            blk = 1 - core if first else core
            for k in range(CHUNKS):
                def part():
                    return lax.dot_general(dz[k, blk].reshape(16 * r32, NBLK), acts[k].reshape(16 * r32, depth),
                                           (((0,), (0,)), ((), ())), preferred_element_type=F32)

                if k == 0:
                    dwp[blk] = part()
                else:
                    dwp[blk] += part()
                if k < CHUNKS - 1:
                    yield
            if first:
                cp = copy(dwp.at[blk], s["dwrx"], other)
            yield
        cp.wait_recv()
        s["dwo"][...] = dwp[core, 0:vloc, :] + s["dwrx"][0:vloc, :]
        shared["o"] = pltpu.make_async_copy(s["dwo"], dw_ref, s["loc_sem"].at[5])
        shared["o"].start()
        yield

    def red_proc():
        redbuf, redrx = s["redbuf"], s["redrx"]
        total_w = _rowsum(ssum[0, 1:] + ssum[1, 1:])
        redbuf[0, :, :depth] = _colsum(s["dgacc"][...])
        lsum = jnp.sum(s["accl"][...]) * (1.0 / 64.0) - jnp.sum(s["acct"][...] / total_w)
        redbuf[0, :, depth:] = jnp.broadcast_to(lsum.reshape(1, 1), (1, 256))
        cp = copy(redbuf.at[0], redrx.at[0], other)
        yield
        cp.wait_recv()
        redbuf[1] = redbuf[0] + redrx[0]
        for i, dims in enumerate(((0, 1), (2,))):
            offs = _around(*dims)
            rx = redrx.at[pl.ds(15 * i + 1, len(offs))]
            g = Group()
            for j, o in enumerate(offs):
                g.add(redbuf.at[1 + i], rx.at[j], peer(o))
            yield
            g.wait_recv()
            redbuf[2 + i] = redbuf[1 + i] + jnp.sum(rx[...], axis=0)
        red_ref[...] = redbuf[3]

    _interleave([chunk(k) for k in range(CHUNKS)] + [w_proc(), red_proc(), dw_proc()])
    shared["o"].wait()
    for c in groups:
        c.wait_send()


def _finish(red_ref, dh_ref, dw_ref, loss_out, dh_out, dw_out, dg_out, redv, dhv, buf, lossv, dgv, sem):
    step = buf.shape[1] // 4
    cols = [(slice(None), pl.ds(i * step, step)) for i in range(4)]
    moves = [(red_ref, redv, None)] + [(dw_ref.at[c], buf.at[c], dw_out.at[c]) for c in cols] + [(dh_ref, dhv, dh_out)]
    gets = [pltpu.make_async_copy(a, b, sem.at[i, 0]) for i, (a, b, _) in enumerate(moves)]
    puts = [pltpu.make_async_copy(b, c, sem.at[i, 1]) for i, (_, b, c) in enumerate(moves) if c is not None]
    for g in gets:
        g.start()
    gets[0].wait()
    lossv[...] = redv[:, dgv.shape[1]:dgv.shape[1] + 1]
    dgv[...] = redv[:, :dgv.shape[1]]
    puts += [pltpu.make_async_copy(lossv, loss_out, sem.at[0, 1]), pltpu.make_async_copy(dgv, dg_out, sem.at[6, 1])]
    for p in puts[5:]:
        p.start()
    for g, p in zip(gets[1:], puts):
        g.wait()
        p.start()
    for p in puts:
        p.wait()


def solution(mesh):
    def local_step(hidden, labels, loss_weight, norm_gain, w_local):
        rows, depth = hidden.shape
        vloc = w_local.shape[1]
        vreal = vloc * mesh.shape["vp"] - PAD_COLS
        vm = pl.BlockSpec(memory_space=pltpu.VMEM)
        hbm = pl.BlockSpec(memory_space=pl.ANY)
        scratch = _scratch(rows, depth, vloc)
        red, dh, dwt = pl.pallas_call(
            functools.partial(_kernel, (rows, depth, vloc, vreal), tuple(scratch)),
            name="head_step",
            out_shape=(jax.ShapeDtypeStruct((1, depth + 256), F32),
                       jax.ShapeDtypeStruct((rows, depth), BF16),
                       jax.ShapeDtypeStruct((vloc, depth), F32)),
            in_specs=[hbm] * 5,
            out_specs=(vm, vm, hbm),
            scratch_shapes=list(scratch.values()),
            compiler_params=pltpu.CompilerParams(
                collective_id=0, has_side_effects=True, vmem_limit_bytes=63 * 1024 * 1024),
        )(labels.reshape(1, rows), loss_weight.reshape(1, rows), hidden, norm_gain.reshape(1, depth), w_local.T)
        loss, dh, dwt, dg = pl.pallas_call(
            _finish,
            name="head_out",
            out_shape=(jax.ShapeDtypeStruct((1, 1), F32),
                       jax.ShapeDtypeStruct((rows, depth), BF16),
                       jax.ShapeDtypeStruct((vloc, depth), F32),
                       jax.ShapeDtypeStruct((1, depth), F32)),
            in_specs=[hbm] * 3,
            out_specs=[hbm] * 4,
            scratch_shapes=[pltpu.VMEM((1, depth + 256), F32), pltpu.VMEM((rows, depth), BF16),
                            pltpu.VMEM((vloc, depth), F32), pltpu.VMEM((1, 1), F32), pltpu.VMEM((1, depth), F32),
                            pltpu.SemaphoreType.DMA((7, 2))],
        )(red, dh, dwt)
        return loss.reshape(1), dh, dwt.T, dg.reshape(depth)

    return jax.shard_map(
        local_step,
        mesh=mesh,
        in_specs=(P(("dp", "vp"), None), P(("dp", "vp")), P(("dp", "vp")), P(None), P(None, "vp")),
        out_specs=(P("dp"), P(("dp", "vp"), None), P("dp", "vp"), P("dp")),
        check_vma=False,
    )
```

```python
import functools
import math
import math

import jax
import jax.numpy as jnp
from jax import lax
from jax.experimental import pallas as pl
from jax.experimental.pallas import tpu as pltpu
from jax.sharding import PartitionSpec as P

NORM_EPS = 1e-5
PAD_COLS = 128
CHUNKS = 4
NBLK = 512
MESH = pl.DeviceIdType.MESH
F32 = jnp.float32
BF16 = jnp.bfloat16
AROUND = (1, 3, 2)
ORDER = (
    "04242133103120210000322221111033233102310236616666002636",
    "621135320153012530123012",
)
UNIT = 16384
DIRECT = (0, 1, 2, 3)


def _around(*dims):
    offs = [{}]
    for d in dims:
        offs = [{**o, d: t} for t in (*AROUND, 0) for o in offs]
    return [o for o in offs if any(o.values())]


def _parts(depth, k):
    tiles = depth // 128
    sizes = [tiles // 3 + (1 if i < tiles % 3 else 0) for i in range(3)]
    sizes = [sizes[(i + k) % 3] for i in range(3)]
    starts = [0, sizes[0], sizes[0] + sizes[1]]
    return tuple((a * 128, n * 128) for a, n in zip(starts, sizes))


def _rowsum(x):
    return jnp.sum(x, axis=1, keepdims=True)


def _colsum(x):
    return jnp.sum(x, axis=0, keepdims=True)


def _scratch(rows, depth, vloc):
    r = rows // CHUNKS
    v = pltpu.VMEM
    c = CHUNKS
    s = {
        "xs": v((c, 4, 4, 4, r, depth), BF16),
        "acts": v((c, 4, 4, 4 * r, depth), BF16),
        "meta": v((4, 4, 4, 2, 128), F32),
        "win": v((vloc, depth), BF16),
        "w2": v((2, NBLK, depth), BF16),
        "ex": v((c, 2, 4, 4, 4, r, NBLK), F32),
        "dz": v((c, 2, 4, 4, 4 * r, NBLK), BF16),
        "gp": v((c, 4, 4, 4, r, depth), F32),
        "dwp": v((2, NBLK, depth), F32),
        "dwrx": v((NBLK, depth), F32),
        "dwo": v((vloc, depth), F32),
        "labc": v((c, 4, 4, 4 * r, 1), F32),
        "wtc": v((c, 4, 4, 4 * r, 1), F32),
        "rcol": v((c, 4, 4, 4 * r, 1), F32),
        "frow": v((c, 4, 1, 128), F32),
        "lrow": v((c, 4, 1, 128), F32),
        "stat": v((c, 3, 4, 1, 128), F32),
        "mloc": v((c, 4, 1, 128), F32),
        "statrx": v((c, 18, 4, 1, 128), F32),
        "ssum": v((2, 2, 128), F32),
        "dgacc": v((r, depth), F32),
        "redbuf": v((4, 1, depth + 256), F32),
        "redrx": v((19, 1, depth + 256), F32),
        "acct": v((4 * r, NBLK), F32),
        "accl": v((4 * r, 128), F32),
        "rx3": v((c, 3, r, depth), F32),
        "dum": v((64, UNIT // 2 // depth, depth), BF16),
        "dum1": v((128, 2, 128), F32),
        "hidv": v((rows, depth), BF16),
        "labv": v((1, rows), jnp.int32),
        "wtv": v((1, rows), F32),
        "gainv": v((1, depth), F32),
    }
    for k in range(c):
        for p, (_, w) in enumerate(_parts(depth, k)):
            shape = (2, 4) if p == 1 else (4, 2)
            s[f"rx1_{k}_{p}"] = v((6, *shape, r, w), F32)
            s[f"rx2_{k}_{p}"] = v((3, 4, r, w) if k == c - 1 else (6, 2, r, w), F32)
    n = 96
    s["send_sem"] = pltpu.SemaphoreType.DMA((n,))
    s["recv_sem"] = pltpu.SemaphoreType.DMA((n,))
    s["loc_sem"] = pltpu.SemaphoreType.DMA((6,))
    return s


def _pick(pairs):
    return tuple(pairs.get(d, slice(None)) for d in (2, 1, 0))


def _interleave(procs):
    for i in map(int, "".join(ORDER)):
        next(procs[i], None)
    for p in procs:
        next(p, None)


def _kernel(dims, names, lab_ref, wt_ref, hid_in, gain_in, w_ref, red_ref, dh_ref, dw_ref, *refs):
    rows, depth, vloc, vreal = dims
    s = dict(zip(names, refs))
    r8 = rows // CHUNKS
    r32 = 4 * r8
    xs, acts, meta, w2, ex, dz, gp = (s[n] for n in ("xs", "acts", "meta", "w2", "ex", "dz", "gp"))
    dwp, stat, statrx, ssum = s["dwp"], s["stat"], s["statrx"], s["ssum"]
    me = lax.axis_index("vp")
    core = lax.rem(me, 2)
    chip = me // 2
    pos = (lax.rem(chip, 4), lax.rem(chip // 4, 4), chip // 16)
    stride = (2, 8, 32)
    other = me + 1 - 2 * core
    own = {0: pos[0], 1: pos[1], 2: pos[2]}
    h0, h1 = slice(0, 2), slice(2, 4)

    def at(d, step):
        return lax.rem(pos[d] + step, 4)

    def peer(off):
        return me + sum((at(d, t) - pos[d]) * stride[d] for d, t in off.items())

    groups = []

    class Group:
        def __init__(self):
            self.sems = s["send_sem"].at[len(groups)], s["recv_sem"].at[len(groups)]
            self.size, self.copies, self.got, self.sent = 0, [], False, False
            groups.append(self)

        def add(self, src, dst, device):
            c = pltpu.make_async_remote_copy(
                src_ref=src, dst_ref=dst, send_sem=self.sems[0], recv_sem=self.sems[1],
                device_id={"vp": device}, device_id_type=MESH)
            c.start()
            self.size += math.prod(src.shape) * src.dtype.itemsize
            self.copies.append(c)
            return self

        def _all(self, sem):
            ref = s["dum"] if self.size % UNIT == 0 else s["dum1"]
            unit = math.prod(ref.shape[1:]) * ref.dtype.itemsize
            part = ref.at[pl.ds(0, self.size // unit)]
            return pltpu.make_async_copy(part, part, sem)

        def wait_recv(self):
            self.got = True
            if len(self.copies) == 1:
                self.copies[0].wait_recv()
            else:
                self._all(self.sems[1]).wait()

        def wait_send(self):
            if self.sent:
                return
            self.sent = True
            if len(self.copies) == 1:
                self.copies[0].wait_send()
            else:
                self._all(self.sems[0]).wait()

    def copy(src, dst, device):
        return Group().add(src, dst, device)

    barrier = pltpu.get_barrier_semaphore()
    peers = [peer(o) for d in range(3) for o in _around(d)] + [other]
    for p in peers:
        pl.semaphore_signal(barrier, inc=1, device_id={"vp": p}, device_id_type=MESH)
    hid_ref, lab_v, wt_v, gain_v = (s[n] for n in ("hidv", "labv", "wtv", "gainv"))
    loads = [pltpu.make_async_copy(a, b, s["loc_sem"].at[i]) for i, (a, b) in enumerate(
        ((hid_in, hid_ref), (lab_ref, lab_v), (wt_ref, wt_v), (gain_in, gain_v), (w_ref, s["win"])))]
    for c in loads:
        c.start()
    wload = loads.pop()
    for n in ("dgacc", "acct", "accl"):
        s[n][...] = jnp.zeros_like(s[n])
    for c in loads:
        c.wait()

    for k in range(CHUNKS):
        xs[k, pos[2], pos[1], pos[0]] = hid_ref[k * r8:(k + 1) * r8, :]
    mine = meta.at[pos[2], pos[1], pos[0]]
    mine[...] = jnp.zeros((2, 128), F32)
    mine[0:1, 0:rows] = lab_v[...].astype(F32)
    mine[1:2, 0:rows] = wt_v[...]
    gain = gain_v[...]
    pl.semaphore_wait(barrier, len(peers))

    lane = lax.broadcasted_iota(jnp.int32, (r32, 128), 1)
    row = lax.broadcasted_iota(jnp.int32, (r32, 128), 0)
    lane_n = lax.broadcasted_iota(jnp.int32, (r32, NBLK), 1)
    bases = [(2 * chip + b) * vloc for b in range(2)]
    shared = {}

    def mview(pairs):
        return meta.at[_pick(pairs)]

    def order(p):
        return p, (p + 1) % 3, (p + 2) % 3

    def half_mat(fn):
        lax.fori_loop(0, 2, lambda i, _: (fn(i), 0)[1], 0)

    def w_proc():
        yield
        wload.wait()
        w2[core, 0:vloc, :] = s["win"][...]
        w2[core, vloc:, :] = jnp.zeros((NBLK - vloc, depth), BF16)
        shared["w"] = copy(w2.at[core], w2.at[core], other)
        yield

    def chunk(k):
        parts = _parts(depth, k)
        last = k == CHUNKS - 1

        def xsl(c, pairs):
            return xs.at[(k, *_pick(pairs), slice(None), pl.ds(*c))]

        def spread(group, view, pairs, dims, src=None):
            ref = view(pairs) if src is None else src
            for o in _around(*dims):
                group.add(ref, view(pairs), peer(o))

        def views(p):
            return [functools.partial(xsl, parts[p])] + [mview] * (p + k == 0)

        def fresh():
            flight[:] = [Group() for _ in range(1 if k else 2)]
            return flight

        def settle():
            for cp in flight:
                cp.wait_recv()

        flight = []
        if k:
            yield
        fresh()
        for p, c in enumerate(parts):
            dims = order(p)[:1]
            spread(flight[0], views(p)[0], own, dims, hid_ref.at[pl.ds(k * r8, r8), pl.ds(*c)])
            for vw in views(p)[1:]:
                spread(flight[1], vw, own, dims)
        yield
        settle()
        fresh()
        for p in range(3):
            _, d, d2 = order(p)
            for i, vw in enumerate(views(p)):
                spread(flight[i], vw, {d: pos[d], d2: pos[d2]}, (d,))
        yield
        settle()
        direct = k in DIRECT
        if not direct:
            ring = [Group(), Group()]
        else:
            fresh()
        for p in range(3):
            _, _, d = order(p)
            for i, vw in enumerate(views(p)):
                if direct:
                    spread(flight[i], vw, {d: pos[d]}, (d,))
                else:
                    src = vw({d: pos[d]})
                    for g, t in zip(ring, (1, 3)):
                        g.add(src, src, peer({d: t}))
        yield
        if not direct:
            fresh()
            for g, t, h in zip(ring, (1, 3), (h0, h1)):
                g.wait_recv()
                for p, c in enumerate(parts):
                    d0, _, d = order(p)
                    vv = xsl(c, {d: at(d, 4 - t), d0: h})
                    flight[0].add(vv, vv, peer({d: t}))
        if not direct:
            yield
        settle()

        def norm(z, _):
            for y in range(4):
                x = xs[k, z, y].astype(F32).reshape(r32, depth)
                inv = lax.rsqrt(jnp.mean(x * x, axis=-1, keepdims=True) + NORM_EPS)
                s["rcol"][k, z, y] = inv
                acts[k, z, y] = (x * inv * gain).astype(BF16)
            return 0

        lax.fori_loop(0, 4, norm, 0)
        if k == 0:
            ssum[0] = jnp.sum(meta[...].reshape(64, 2, 128), axis=0)
            shared["s"] = copy(ssum.at[0], ssum.at[1], other)
            shared["w"].wait_recv()
        yield

        def zdot(i):
            a = acts[k, pl.ds(2 * i, 2)].reshape(8 * r32, depth)
            for b in range(2):
                ex[k, b, pl.ds(2 * i, 2)] = lax.dot_general(
                    a, w2[b], (((1,), (1,)), ((), ())),
                    preferred_element_type=F32).reshape(2, 4, 4, r8, NBLK)

        zdot(0)
        yield

        def soft(z, _):
            mrow = jnp.zeros((1, 128), F32)
            srow = jnp.zeros((1, 128), F32)
            for y in range(4):
                def col(j):
                    m = jnp.broadcast_to(meta[z, y, :, j:j + 1, :], (4, r8, 128)).reshape(r32, 128)
                    return _rowsum(jnp.where(lane == k * r8 + lax.rem(row, r8), m, 0.0))

                lab, wt = col(0), col(1)
                s["labc"][k, z, y] = lab
                s["wtc"][k, z, y] = wt
                labi = lab.astype(jnp.int32)
                vals = []
                tgt = jnp.zeros((r32, NBLK), F32)
                for b in range(2):
                    val = ex[k, b, z, y].reshape(r32, NBLK)
                    ok = (lane_n < vloc) & (lane_n < vreal - bases[b])
                    tgt = tgt + jnp.where((lane_n == labi - bases[b]) & (lane_n < vloc), val, 0.0)
                    vals.append(jnp.where(ok, val, -jnp.inf))
                mx = jnp.max(jnp.maximum(vals[0], vals[1]), axis=1, keepdims=True)
                es = [jnp.exp(val - mx) for val in vals]
                sm = _rowsum(es[0] + es[1])
                for b in range(2):
                    ex[k, b, z, y] = es[b].reshape(4, r8, NBLK)
                here = lane == row + r32 * y
                mrow = mrow + _colsum(jnp.where(here, mx, 0.0))
                srow = srow + _colsum(jnp.where(here, sm, 0.0))
                s["acct"][...] += tgt * wt
            s["mloc"][k, z] = mrow
            stat[k, 0, z] = mrow + jnp.log(srow)
            return 0

        zdot(1)
        soft(0, 0)
        soft(1, 0)
        yield
        soft(2, 0)
        soft(3, 0)
        for i, dims in enumerate(((0, 1), (2,))):
            offs = _around(*dims)
            rx = statrx.at[k, pl.ds(15 * i, len(offs))]
            g = Group()
            for j, o in enumerate(offs):
                g.add(stat.at[k, i], rx.at[j], peer(o))
            yield
            g.wait_recv()
            mine = stat[k, i]
            got = rx[...]
            top = jnp.maximum(mine, jnp.max(got, axis=0))
            stat[k, i + 1] = top + jnp.log(jnp.exp(mine - top) + jnp.sum(jnp.exp(got - top), axis=0))
        lse = stat[k, 2]
        s["lrow"][k] = lse
        s["frow"][k] = jnp.exp(s["mloc"][k] - lse)
        if k == 0:
            shared["s"].wait_recv()
        total_w = _rowsum(ssum[0, 1:] + ssum[1, 1:])

        def grad(z, _):
            for y in range(4):
                here = lane == row + r32 * y
                fr = jnp.broadcast_to(s["frow"][k, z], (r32, 128))
                lr = jnp.broadcast_to(s["lrow"][k, z], (r32, 128))
                fc = _rowsum(jnp.where(here, fr, 0.0))
                lab = s["labc"][k, z, y].astype(jnp.int32)
                sc = s["wtc"][k, z, y] / total_w
                s["accl"][...] += jnp.where(here, lr, 0.0) * sc
                for b in range(2):
                    prob = ex[k, b, z, y].reshape(r32, NBLK) * fc
                    hit = (lane_n == lab - bases[b]) & (lane_n < vloc)
                    dz[k, b, z, y] = ((prob - jnp.where(hit, 1.0, 0.0)) * sc).astype(BF16)
            return 0


        def gdot(i):
            zz = pl.ds(2 * i, 2)
            g = jnp.dot(dz[k, 0, zz].reshape(8 * r32, NBLK), w2[0], preferred_element_type=F32)
            g = g + jnp.dot(dz[k, 1, zz].reshape(8 * r32, NBLK), w2[1], preferred_element_type=F32)
            gp[k, zz] = g.reshape(2, 4, 4, r8, depth)

        for i in range(2):
            grad(2 * i, 0)
            grad(2 * i + 1, 0)
            gdot(i)

        def gsl(c, pairs):
            return gp.at[(k, *_pick(pairs), slice(None), pl.ds(*c))]

        def rs_far(bufs, c, d, hd, base, gs):
            for i, (g, h, t) in enumerate(zip(gs, (h0, h1), (1, 3))):
                g.add(gsl(c, {**base, d: at(d, 2), hd: h}), bufs.at[i], peer({d: t}))

        def rs_near(bufs, c, d, hd, base, gs):
            for i, (h, t) in enumerate(zip((h1, h0), (1, 3))):
                gs[2].add(gsl(c, {**base, d: at(d, t), hd: h}), bufs.at[2 + i], peer({d: t}))

        def triple():
            return [Group() for _ in range(3)]

        def rs_relay(todo, gs):
            for i, t in enumerate((1, 3)):
                gs[i].wait_recv()
                for bufs, c, d, hd, _, base in todo:
                    bufs[i] += gp[(k, *_pick({**base, d: at(d, t), hd: (h0, h1)[i]}), slice(None), pl.ds(*c))]
                    gs[2].add(bufs.at[i], bufs.at[4 + i], peer({d: t}))

        def rs_finish(bufs, c, d, hd, _, base):
            for h, k1, k2 in ((h0, 3, 4), (h1, 2, 5)):
                sl = (k, *_pick({**base, d: pos[d], hd: h}), slice(None), pl.ds(*c))
                gp[sl] = gp[sl] + (bufs[k1] + bufs[k2])

        rx1 = [s[f"rx1_{k}_{p}"] for p in range(3)]
        rx2 = [s[f"rx2_{k}_{p}"] for p in range(3)]
        todo1 = [(rx1[p], c, *order(p), {}) for p, c in enumerate(parts)]
        todo2 = [(rx2[p], c, order(p)[1], order(p)[2], None, {p: pos[p]}) for p, c in enumerate(parts)]
        gs1 = triple()
        for bufs, c, d, hd, _, base in todo1:
            rs_far(bufs, c, d, hd, base, gs1)
        yield
        for bufs, c, d, hd, _, base in todo1:
            rs_near(bufs, c, d, hd, base, gs1)
        yield

        def dg(z, _):
            acc = jnp.zeros((r8, depth), F32)
            for y in range(4):
                n = xs[k, z, y].astype(F32).reshape(r32, depth) * s["rcol"][k, z, y]
                t = gp[k, z, y].reshape(r32, depth) * n
                acc = acc + jnp.sum(t.reshape(4, r8, depth), axis=0)
            s["dgacc"][...] += acc
            return 0

        lax.fori_loop(0, 4, dg, 0)
        yield
        rs_relay(todo1, gs1)
        yield
        gs1[2].wait_recv()
        gs2 = [Group()] if last else triple()
        for t1, (bufs, c, d, hd, _, base) in zip(todo1, todo2):
            rs_finish(*t1)
            if last:
                for i, t in enumerate(AROUND):
                    gs2[0].add(gsl(c, {**base, d: at(d, t)}), bufs.at[i], peer({d: t}))
            else:
                rs_far(bufs, c, d, hd, base, gs2)
                rs_near(bufs, c, d, hd, base, gs2)
        yield
        if last:
            gs2[0].wait_recv()
            for bufs, c, d, _, _, base in todo2:
                sl = (k, *_pick({**base, d: pos[d]}), slice(None), pl.ds(*c))
                gp[sl] = (gp[sl] + bufs[0]) + (bufs[1] + bufs[2])
        else:
            rs_relay(todo2, gs2)
            yield
            gs2[2].wait_recv()
            for t2 in todo2:
                rs_finish(*t2)
        g3 = Group()
        for _, c, d1, d, _, base in todo2:
            for i, t in enumerate(AROUND):
                g3.add(gsl(c, {**base, d1: pos[d1], d: at(d, t)}), s["rx3"].at[k, i, :, pl.ds(*c)], peer({d: t}))
        yield
        if last:
            for g in groups:
                if g.got:
                    g.wait_send()
        g3.wait_recv()
        g = gp[k, pos[2], pos[1], pos[0]]
        for i in range(3):
            g = g + s["rx3"][k, i]
        x = hid_ref[k * r8:(k + 1) * r8, :].astype(F32)
        inv = lax.rsqrt(jnp.mean(x * x, axis=-1, keepdims=True) + NORM_EPS)
        n = x * inv
        u = g * gain
        dh_ref[k * r8:(k + 1) * r8, :] = (inv * (u - n * jnp.mean(u * n, axis=-1, keepdims=True))).astype(BF16)
        yield

    def dw_proc():
        for first in (True, False):
            blk = 1 - core if first else core
            for k in range(CHUNKS):
                def part():
                    return lax.dot_general(dz[k, blk].reshape(16 * r32, NBLK), acts[k].reshape(16 * r32, depth),
                                           (((0,), (0,)), ((), ())), preferred_element_type=F32)

                if k == 0:
                    dwp[blk] = part()
                else:
                    dwp[blk] += part()
                if k < CHUNKS - 1:
                    yield
            if first:
                cp = copy(dwp.at[blk], s["dwrx"], other)
            yield
        cp.wait_recv()
        s["dwo"][...] = dwp[core, 0:vloc, :] + s["dwrx"][0:vloc, :]
        shared["o"] = pltpu.make_async_copy(s["dwo"], dw_ref, s["loc_sem"].at[5])
        shared["o"].start()
        yield

    def red_proc():
        redbuf, redrx = s["redbuf"], s["redrx"]
        total_w = _rowsum(ssum[0, 1:] + ssum[1, 1:])
        redbuf[0, :, :depth] = _colsum(s["dgacc"][...])
        lsum = jnp.sum(s["accl"][...]) * (1.0 / 64.0) - jnp.sum(s["acct"][...] / total_w)
        redbuf[0, :, depth:] = jnp.broadcast_to(lsum.reshape(1, 1), (1, 256))
        cp = copy(redbuf.at[0], redrx.at[0], other)
        yield
        cp.wait_recv()
        redbuf[1] = redbuf[0] + redrx[0]
        for i, dims in enumerate(((0, 1), (2,))):
            offs = _around(*dims)
            rx = redrx.at[pl.ds(15 * i + 1, len(offs))]
            g = Group()
            for j, o in enumerate(offs):
                g.add(redbuf.at[1 + i], rx.at[j], peer(o))
            yield
            g.wait_recv()
            redbuf[2 + i] = redbuf[1 + i] + jnp.sum(rx[...], axis=0)
        red_ref[...] = redbuf[3]

    _interleave([chunk(k) for k in range(CHUNKS)] + [w_proc(), red_proc(), dw_proc()])
    shared["o"].wait()
    for c in groups:
        c.wait_send()


def _finish(red_ref, dh_ref, dw_ref, loss_out, dh_out, dw_out, dg_out, redv, dhv, buf, lossv, dgv, sem):
    step = buf.shape[1] // 4
    cols = [(slice(None), pl.ds(i * step, step)) for i in range(4)]
    moves = [(red_ref, redv, None)] + [(dw_ref.at[c], buf.at[c], dw_out.at[c]) for c in cols] + [(dh_ref, dhv, dh_out)]
    gets = [pltpu.make_async_copy(a, b, sem.at[i, 0]) for i, (a, b, _) in enumerate(moves)]
    puts = [pltpu.make_async_copy(b, c, sem.at[i, 1]) for i, (_, b, c) in enumerate(moves) if c is not None]
    for g in gets:
        g.start()
    gets[0].wait()
    lossv[...] = redv[:, dgv.shape[1]:dgv.shape[1] + 1]
    dgv[...] = redv[:, :dgv.shape[1]]
    puts += [pltpu.make_async_copy(lossv, loss_out, sem.at[0, 1]), pltpu.make_async_copy(dgv, dg_out, sem.at[6, 1])]
    for p in puts[5:]:
        p.start()
    for g, p in zip(gets[1:], puts):
        g.wait()
        p.start()
    for p in puts:
        p.wait()


def solution(mesh):
    def local_step(hidden, labels, loss_weight, norm_gain, w_local):
        rows, depth = hidden.shape
        vloc = w_local.shape[1]
        vreal = vloc * mesh.shape["vp"] - PAD_COLS
        vm = pl.BlockSpec(memory_space=pltpu.VMEM)
        hbm = pl.BlockSpec(memory_space=pl.ANY)
        scratch = _scratch(rows, depth, vloc)
        red, dh, dwt = pl.pallas_call(
            functools.partial(_kernel, (rows, depth, vloc, vreal), tuple(scratch)),
            name="head_step",
            out_shape=(jax.ShapeDtypeStruct((1, depth + 256), F32),
                       jax.ShapeDtypeStruct((rows, depth), BF16),
                       jax.ShapeDtypeStruct((vloc, depth), F32)),
            in_specs=[hbm] * 5,
            out_specs=(vm, vm, hbm),
            scratch_shapes=list(scratch.values()),
            compiler_params=pltpu.CompilerParams(
                collective_id=0, has_side_effects=True, vmem_limit_bytes=63 * 1024 * 1024),
        )(labels.reshape(1, rows), loss_weight.reshape(1, rows), hidden, norm_gain.reshape(1, depth), w_local.T)
        loss, dh, dwt, dg = pl.pallas_call(
            _finish,
            name="head_out",
            out_shape=(jax.ShapeDtypeStruct((1, 1), F32),
                       jax.ShapeDtypeStruct((rows, depth), BF16),
                       jax.ShapeDtypeStruct((vloc, depth), F32),
                       jax.ShapeDtypeStruct((1, depth), F32)),
            in_specs=[hbm] * 3,
            out_specs=[hbm] * 4,
            scratch_shapes=[pltpu.VMEM((1, depth + 256), F32), pltpu.VMEM((rows, depth), BF16),
                            pltpu.VMEM((vloc, depth), F32), pltpu.VMEM((1, 1), F32), pltpu.VMEM((1, depth), F32),
                            pltpu.SemaphoreType.DMA((7, 2))],
        )(red, dh, dwt)
        return loss.reshape(1), dh, dwt.T, dg.reshape(depth)

    return jax.shard_map(
        local_step,
        mesh=mesh,
        in_specs=(P(("dp", "vp"), None), P(("dp", "vp")), P(("dp", "vp")), P(None), P(None, "vp")),
        out_specs=(P("dp"), P(("dp", "vp"), None), P("dp", "vp"), P("dp")),
        check_vma=False,
    )
```

```python
import functools
import math
import math

import jax
import jax.numpy as jnp
from jax import lax
from jax.experimental import pallas as pl
from jax.experimental.pallas import tpu as pltpu
from jax.sharding import PartitionSpec as P

NORM_EPS = 1e-5
PAD_COLS = 128
CHUNKS = 4
NBLK = 512
MESH = pl.DeviceIdType.MESH
F32 = jnp.float32
BF16 = jnp.bfloat16
AROUND = (1, 3, 2)
ORDER = (
    "01342423101230210000322221110133233012301366206166360626",
    "261135320153201532013201",
)
UNIT = 16384
DIRECT = (0, 1, 2, 3)


def _around(*dims):
    offs = [{}]
    for d in dims:
        offs = [{**o, d: t} for t in (*AROUND, 0) for o in offs]
    return [o for o in offs if any(o.values())]


def _parts(depth, k):
    tiles = depth // 128
    sizes = [tiles // 3 + (1 if i < tiles % 3 else 0) for i in range(3)]
    sizes = [sizes[(i + k) % 3] for i in range(3)]
    starts = [0, sizes[0], sizes[0] + sizes[1]]
    return tuple((a * 128, n * 128) for a, n in zip(starts, sizes))


def _rowsum(x):
    return jnp.sum(x, axis=1, keepdims=True)


def _colsum(x):
    return jnp.sum(x, axis=0, keepdims=True)


def _scratch(rows, depth, vloc):
    r = rows // CHUNKS
    v = pltpu.VMEM
    c = CHUNKS
    s = {
        "xs": v((c, 4, 4, 4, r, depth), BF16),
        "acts": v((c, 4, 4, 4 * r, depth), BF16),
        "meta": v((4, 4, 4, 2, 128), F32),
        "win": v((vloc, depth), BF16),
        "w2": v((2, NBLK, depth), BF16),
        "ex": v((c, 2, 4, 4, 4, r, NBLK), F32),
        "dz": v((c, 2, 4, 4, 4 * r, NBLK), BF16),
        "gp": v((c, 4, 4, 4, r, depth), F32),
        "dwp": v((2, NBLK, depth), F32),
        "dwrx": v((NBLK, depth), F32),
        "dwo": v((vloc, depth), F32),
        "labc": v((c, 4, 4, 4 * r, 1), F32),
        "wtc": v((c, 4, 4, 4 * r, 1), F32),
        "rcol": v((c, 4, 4, 4 * r, 1), F32),
        "frow": v((c, 4, 1, 128), F32),
        "lrow": v((c, 4, 1, 128), F32),
        "stat": v((c, 3, 4, 1, 128), F32),
        "mloc": v((c, 4, 1, 128), F32),
        "statrx": v((c, 18, 4, 1, 128), F32),
        "ssum": v((2, 2, 128), F32),
        "dgacc": v((r, depth), F32),
        "redbuf": v((4, 1, depth + 256), F32),
        "redrx": v((19, 1, depth + 256), F32),
        "acct": v((4 * r, NBLK), F32),
        "accl": v((4 * r, 128), F32),
        "rx3": v((c, 3, r, depth), F32),
        "dum": v((64, UNIT // 2 // depth, depth), BF16),
        "dum1": v((128, 2, 128), F32),
        "hidv": v((rows, depth), BF16),
        "labv": v((1, rows), jnp.int32),
        "wtv": v((1, rows), F32),
        "gainv": v((1, depth), F32),
    }
    for k in range(c):
        for p, (_, w) in enumerate(_parts(depth, k)):
            shape = (2, 4) if p == 1 else (4, 2)
            s[f"rx1_{k}_{p}"] = v((6, *shape, r, w), F32)
            s[f"rx2_{k}_{p}"] = v((3, 4, r, w) if k == c - 1 else (6, 2, r, w), F32)
    n = 96
    s["send_sem"] = pltpu.SemaphoreType.DMA((n,))
    s["recv_sem"] = pltpu.SemaphoreType.DMA((n,))
    s["loc_sem"] = pltpu.SemaphoreType.DMA((6,))
    return s


def _pick(pairs):
    return tuple(pairs.get(d, slice(None)) for d in (2, 1, 0))


def _interleave(procs):
    for i in map(int, "".join(ORDER)):
        next(procs[i], None)
    for p in procs:
        next(p, None)


def _kernel(dims, names, lab_ref, wt_ref, hid_in, gain_in, w_ref, red_ref, dh_ref, dw_ref, *refs):
    rows, depth, vloc, vreal = dims
    s = dict(zip(names, refs))
    r8 = rows // CHUNKS
    r32 = 4 * r8
    xs, acts, meta, w2, ex, dz, gp = (s[n] for n in ("xs", "acts", "meta", "w2", "ex", "dz", "gp"))
    dwp, stat, statrx, ssum = s["dwp"], s["stat"], s["statrx"], s["ssum"]
    me = lax.axis_index("vp")
    core = lax.rem(me, 2)
    chip = me // 2
    pos = (lax.rem(chip, 4), lax.rem(chip // 4, 4), chip // 16)
    stride = (2, 8, 32)
    other = me + 1 - 2 * core
    own = {0: pos[0], 1: pos[1], 2: pos[2]}
    h0, h1 = slice(0, 2), slice(2, 4)

    def at(d, step):
        return lax.rem(pos[d] + step, 4)

    def peer(off):
        return me + sum((at(d, t) - pos[d]) * stride[d] for d, t in off.items())

    groups = []

    class Group:
        def __init__(self):
            self.sems = s["send_sem"].at[len(groups)], s["recv_sem"].at[len(groups)]
            self.size, self.copies, self.got, self.sent = 0, [], False, False
            groups.append(self)

        def add(self, src, dst, device):
            c = pltpu.make_async_remote_copy(
                src_ref=src, dst_ref=dst, send_sem=self.sems[0], recv_sem=self.sems[1],
                device_id={"vp": device}, device_id_type=MESH)
            c.start()
            self.size += math.prod(src.shape) * src.dtype.itemsize
            self.copies.append(c)
            return self

        def _all(self, sem):
            ref = s["dum"] if self.size % UNIT == 0 else s["dum1"]
            unit = math.prod(ref.shape[1:]) * ref.dtype.itemsize
            part = ref.at[pl.ds(0, self.size // unit)]
            return pltpu.make_async_copy(part, part, sem)

        def wait_recv(self):
            self.got = True
            if len(self.copies) == 1:
                self.copies[0].wait_recv()
            else:
                self._all(self.sems[1]).wait()

        def wait_send(self):
            if self.sent:
                return
            self.sent = True
            if len(self.copies) == 1:
                self.copies[0].wait_send()
            else:
                self._all(self.sems[0]).wait()

    def copy(src, dst, device):
        return Group().add(src, dst, device)

    barrier = pltpu.get_barrier_semaphore()
    peers = [peer(o) for d in range(3) for o in _around(d)] + [other]
    for p in peers:
        pl.semaphore_signal(barrier, inc=1, device_id={"vp": p}, device_id_type=MESH)
    hid_ref, lab_v, wt_v, gain_v = (s[n] for n in ("hidv", "labv", "wtv", "gainv"))
    loads = [pltpu.make_async_copy(a, b, s["loc_sem"].at[i]) for i, (a, b) in enumerate(
        ((hid_in, hid_ref), (lab_ref, lab_v), (wt_ref, wt_v), (gain_in, gain_v), (w_ref, s["win"])))]
    for c in loads:
        c.start()
    wload = loads.pop()
    for n in ("dgacc", "acct", "accl"):
        s[n][...] = jnp.zeros_like(s[n])
    for c in loads:
        c.wait()

    for k in range(CHUNKS):
        xs[k, pos[2], pos[1], pos[0]] = hid_ref[k * r8:(k + 1) * r8, :]
    mine = meta.at[pos[2], pos[1], pos[0]]
    mine[...] = jnp.zeros((2, 128), F32)
    mine[0:1, 0:rows] = lab_v[...].astype(F32)
    mine[1:2, 0:rows] = wt_v[...]
    gain = gain_v[...]
    pl.semaphore_wait(barrier, len(peers))

    lane = lax.broadcasted_iota(jnp.int32, (r32, 128), 1)
    row = lax.broadcasted_iota(jnp.int32, (r32, 128), 0)
    lane_n = lax.broadcasted_iota(jnp.int32, (r32, NBLK), 1)
    bases = [(2 * chip + b) * vloc for b in range(2)]
    shared = {}

    def mview(pairs):
        return meta.at[_pick(pairs)]

    def order(p):
        return p, (p + 1) % 3, (p + 2) % 3

    def half_mat(fn):
        lax.fori_loop(0, 2, lambda i, _: (fn(i), 0)[1], 0)

    def w_proc():
        yield
        wload.wait()
        w2[core, 0:vloc, :] = s["win"][...]
        w2[core, vloc:, :] = jnp.zeros((NBLK - vloc, depth), BF16)
        shared["w"] = copy(w2.at[core], w2.at[core], other)
        yield

    def chunk(k):
        parts = _parts(depth, k)
        last = k == CHUNKS - 1

        def xsl(c, pairs):
            return xs.at[(k, *_pick(pairs), slice(None), pl.ds(*c))]

        def spread(group, view, pairs, dims, src=None):
            ref = view(pairs) if src is None else src
            for o in _around(*dims):
                group.add(ref, view(pairs), peer(o))

        def views(p):
            return [functools.partial(xsl, parts[p])] + [mview] * (p + k == 0)

        def fresh():
            flight[:] = [Group() for _ in range(1 if k else 2)]
            return flight

        def settle():
            for cp in flight:
                cp.wait_recv()

        flight = []
        if k:
            yield
        fresh()
        for p, c in enumerate(parts):
            dims = order(p)[:1]
            spread(flight[0], views(p)[0], own, dims, hid_ref.at[pl.ds(k * r8, r8), pl.ds(*c)])
            for vw in views(p)[1:]:
                spread(flight[1], vw, own, dims)
        yield
        settle()
        fresh()
        for p in range(3):
            _, d, d2 = order(p)
            for i, vw in enumerate(views(p)):
                spread(flight[i], vw, {d: pos[d], d2: pos[d2]}, (d,))
        yield
        settle()
        direct = k in DIRECT
        if not direct:
            ring = [Group(), Group()]
        else:
            fresh()
        for p in range(3):
            _, _, d = order(p)
            for i, vw in enumerate(views(p)):
                if direct:
                    spread(flight[i], vw, {d: pos[d]}, (d,))
                else:
                    src = vw({d: pos[d]})
                    for g, t in zip(ring, (1, 3)):
                        g.add(src, src, peer({d: t}))
        yield
        if not direct:
            fresh()
            for g, t, h in zip(ring, (1, 3), (h0, h1)):
                g.wait_recv()
                for p, c in enumerate(parts):
                    d0, _, d = order(p)
                    vv = xsl(c, {d: at(d, 4 - t), d0: h})
                    flight[0].add(vv, vv, peer({d: t}))
        if not direct:
            yield
        settle()

        def norm(z, _):
            for y in range(4):
                x = xs[k, z, y].astype(F32).reshape(r32, depth)
                inv = lax.rsqrt(jnp.mean(x * x, axis=-1, keepdims=True) + NORM_EPS)
                s["rcol"][k, z, y] = inv
                acts[k, z, y] = (x * inv * gain).astype(BF16)
            return 0

        norm(0, 0)
        norm(1, 0)
        if k == 0:
            ssum[0] = jnp.sum(meta[...].reshape(64, 2, 128), axis=0)
            shared["s"] = copy(ssum.at[0], ssum.at[1], other)
            shared["w"].wait_recv()
        yield

        def zdot(i):
            a = acts[k, pl.ds(2 * i, 2)].reshape(8 * r32, depth)
            for b in range(2):
                ex[k, b, pl.ds(2 * i, 2)] = lax.dot_general(
                    a, w2[b], (((1,), (1,)), ((), ())),
                    preferred_element_type=F32).reshape(2, 4, 4, r8, NBLK)

        zdot(0)
        norm(2, 0)
        norm(3, 0)
        yield

        def soft(z, _):
            mrow = jnp.zeros((1, 128), F32)
            srow = jnp.zeros((1, 128), F32)
            for y in range(4):
                def col(j):
                    m = jnp.broadcast_to(meta[z, y, :, j:j + 1, :], (4, r8, 128)).reshape(r32, 128)
                    return _rowsum(jnp.where(lane == k * r8 + lax.rem(row, r8), m, 0.0))

                lab, wt = col(0), col(1)
                s["labc"][k, z, y] = lab
                s["wtc"][k, z, y] = wt
                labi = lab.astype(jnp.int32)
                vals = []
                tgt = jnp.zeros((r32, NBLK), F32)
                for b in range(2):
                    val = ex[k, b, z, y].reshape(r32, NBLK)
                    ok = (lane_n < vloc) & (lane_n < vreal - bases[b])
                    tgt = tgt + jnp.where((lane_n == labi - bases[b]) & (lane_n < vloc), val, 0.0)
                    vals.append(jnp.where(ok, val, -jnp.inf))
                mx = jnp.max(jnp.maximum(vals[0], vals[1]), axis=1, keepdims=True)
                es = [jnp.exp(val - mx) for val in vals]
                sm = _rowsum(es[0] + es[1])
                for b in range(2):
                    ex[k, b, z, y] = es[b].reshape(4, r8, NBLK)
                here = lane == row + r32 * y
                mrow = mrow + _colsum(jnp.where(here, mx, 0.0))
                srow = srow + _colsum(jnp.where(here, sm, 0.0))
                s["acct"][...] += tgt * wt
            s["mloc"][k, z] = mrow
            stat[k, 0, z] = mrow + jnp.log(srow)
            return 0

        zdot(1)
        soft(0, 0)
        soft(1, 0)
        yield
        soft(2, 0)
        soft(3, 0)
        for i, dims in enumerate(((0, 1), (2,))):
            offs = _around(*dims)
            rx = statrx.at[k, pl.ds(15 * i, len(offs))]
            g = Group()
            for j, o in enumerate(offs):
                g.add(stat.at[k, i], rx.at[j], peer(o))
            yield
            g.wait_recv()
            mine = stat[k, i]
            got = rx[...]
            top = jnp.maximum(mine, jnp.max(got, axis=0))
            stat[k, i + 1] = top + jnp.log(jnp.exp(mine - top) + jnp.sum(jnp.exp(got - top), axis=0))
        lse = stat[k, 2]
        s["lrow"][k] = lse
        s["frow"][k] = jnp.exp(s["mloc"][k] - lse)
        if k == 0:
            shared["s"].wait_recv()
        total_w = _rowsum(ssum[0, 1:] + ssum[1, 1:])

        def grad(z, _):
            for y in range(4):
                here = lane == row + r32 * y
                fr = jnp.broadcast_to(s["frow"][k, z], (r32, 128))
                lr = jnp.broadcast_to(s["lrow"][k, z], (r32, 128))
                fc = _rowsum(jnp.where(here, fr, 0.0))
                lab = s["labc"][k, z, y].astype(jnp.int32)
                sc = s["wtc"][k, z, y] / total_w
                s["accl"][...] += jnp.where(here, lr, 0.0) * sc
                for b in range(2):
                    prob = ex[k, b, z, y].reshape(r32, NBLK) * fc
                    hit = (lane_n == lab - bases[b]) & (lane_n < vloc)
                    dz[k, b, z, y] = ((prob - jnp.where(hit, 1.0, 0.0)) * sc).astype(BF16)
            return 0


        def gdot(i):
            zz = pl.ds(2 * i, 2)
            g = jnp.dot(dz[k, 0, zz].reshape(8 * r32, NBLK), w2[0], preferred_element_type=F32)
            g = g + jnp.dot(dz[k, 1, zz].reshape(8 * r32, NBLK), w2[1], preferred_element_type=F32)
            gp[k, zz] = g.reshape(2, 4, 4, r8, depth)

        for i in range(2):
            grad(2 * i, 0)
            grad(2 * i + 1, 0)
            gdot(i)

        def gsl(c, pairs):
            return gp.at[(k, *_pick(pairs), slice(None), pl.ds(*c))]

        def rs_far(bufs, c, d, hd, base, gs):
            for i, (g, h, t) in enumerate(zip(gs, (h0, h1), (1, 3))):
                g.add(gsl(c, {**base, d: at(d, 2), hd: h}), bufs.at[i], peer({d: t}))

        def rs_near(bufs, c, d, hd, base, gs):
            for i, (h, t) in enumerate(zip((h1, h0), (1, 3))):
                gs[2].add(gsl(c, {**base, d: at(d, t), hd: h}), bufs.at[2 + i], peer({d: t}))

        def triple():
            return [Group() for _ in range(3)]

        def rs_relay(todo, gs):
            for i, t in enumerate((1, 3)):
                gs[i].wait_recv()
                for bufs, c, d, hd, _, base in todo:
                    bufs[i] += gp[(k, *_pick({**base, d: at(d, t), hd: (h0, h1)[i]}), slice(None), pl.ds(*c))]
                    gs[2].add(bufs.at[i], bufs.at[4 + i], peer({d: t}))

        def rs_finish(bufs, c, d, hd, _, base):
            for h, k1, k2 in ((h0, 3, 4), (h1, 2, 5)):
                sl = (k, *_pick({**base, d: pos[d], hd: h}), slice(None), pl.ds(*c))
                gp[sl] = gp[sl] + (bufs[k1] + bufs[k2])

        rx1 = [s[f"rx1_{k}_{p}"] for p in range(3)]
        rx2 = [s[f"rx2_{k}_{p}"] for p in range(3)]
        todo1 = [(rx1[p], c, *order(p), {}) for p, c in enumerate(parts)]
        todo2 = [(rx2[p], c, order(p)[1], order(p)[2], None, {p: pos[p]}) for p, c in enumerate(parts)]
        gs1 = triple()
        for bufs, c, d, hd, _, base in todo1:
            rs_far(bufs, c, d, hd, base, gs1)
        yield
        for bufs, c, d, hd, _, base in todo1:
            rs_near(bufs, c, d, hd, base, gs1)
        yield

        def dg(z, _):
            acc = jnp.zeros((r8, depth), F32)
            for y in range(4):
                n = xs[k, z, y].astype(F32).reshape(r32, depth) * s["rcol"][k, z, y]
                t = gp[k, z, y].reshape(r32, depth) * n
                acc = acc + jnp.sum(t.reshape(4, r8, depth), axis=0)
            s["dgacc"][...] += acc
            return 0

        lax.fori_loop(0, 4, dg, 0)
        yield
        rs_relay(todo1, gs1)
        yield
        gs1[2].wait_recv()
        gs2 = [Group()] if last else triple()
        for t1, (bufs, c, d, hd, _, base) in zip(todo1, todo2):
            rs_finish(*t1)
            if last:
                for i, t in enumerate(AROUND):
                    gs2[0].add(gsl(c, {**base, d: at(d, t)}), bufs.at[i], peer({d: t}))
            else:
                rs_far(bufs, c, d, hd, base, gs2)
                rs_near(bufs, c, d, hd, base, gs2)
        yield
        if last:
            gs2[0].wait_recv()
            for bufs, c, d, _, _, base in todo2:
                sl = (k, *_pick({**base, d: pos[d]}), slice(None), pl.ds(*c))
                gp[sl] = (gp[sl] + bufs[0]) + (bufs[1] + bufs[2])
        else:
            rs_relay(todo2, gs2)
            yield
            gs2[2].wait_recv()
            for t2 in todo2:
                rs_finish(*t2)
        g3 = Group()
        for _, c, d1, d, _, base in todo2:
            for i, t in enumerate(AROUND):
                g3.add(gsl(c, {**base, d1: pos[d1], d: at(d, t)}), s["rx3"].at[k, i, :, pl.ds(*c)], peer({d: t}))
        yield
        if last:
            for g in groups:
                if g.got:
                    g.wait_send()
        g3.wait_recv()
        g = gp[k, pos[2], pos[1], pos[0]]
        for i in range(3):
            g = g + s["rx3"][k, i]
        x = hid_ref[k * r8:(k + 1) * r8, :].astype(F32)
        inv = lax.rsqrt(jnp.mean(x * x, axis=-1, keepdims=True) + NORM_EPS)
        n = x * inv
        u = g * gain
        dh_ref[k * r8:(k + 1) * r8, :] = (inv * (u - n * jnp.mean(u * n, axis=-1, keepdims=True))).astype(BF16)
        yield

    def dw_proc():
        for first in (True, False):
            blk = 1 - core if first else core
            for k in range(CHUNKS):
                def part():
                    return lax.dot_general(dz[k, blk].reshape(16 * r32, NBLK), acts[k].reshape(16 * r32, depth),
                                           (((0,), (0,)), ((), ())), preferred_element_type=F32)

                if k == 0:
                    dwp[blk] = part()
                else:
                    dwp[blk] += part()
                if k < CHUNKS - 1:
                    yield
            if first:
                cp = copy(dwp.at[blk], s["dwrx"], other)
            yield
        cp.wait_recv()
        s["dwo"][...] = dwp[core, 0:vloc, :] + s["dwrx"][0:vloc, :]
        shared["o"] = pltpu.make_async_copy(s["dwo"], dw_ref, s["loc_sem"].at[5])
        shared["o"].start()
        yield

    def red_proc():
        redbuf, redrx = s["redbuf"], s["redrx"]
        total_w = _rowsum(ssum[0, 1:] + ssum[1, 1:])
        redbuf[0, :, :depth] = _colsum(s["dgacc"][...])
        lsum = jnp.sum(s["accl"][...]) * (1.0 / 64.0) - jnp.sum(s["acct"][...] / total_w)
        redbuf[0, :, depth:] = jnp.broadcast_to(lsum.reshape(1, 1), (1, 256))
        cp = copy(redbuf.at[0], redrx.at[0], other)
        yield
        cp.wait_recv()
        redbuf[1] = redbuf[0] + redrx[0]
        for i, dims in enumerate(((0, 1), (2,))):
            offs = _around(*dims)
            rx = redrx.at[pl.ds(15 * i + 1, len(offs))]
            g = Group()
            for j, o in enumerate(offs):
                g.add(redbuf.at[1 + i], rx.at[j], peer(o))
            yield
            g.wait_recv()
            redbuf[2 + i] = redbuf[1 + i] + jnp.sum(rx[...], axis=0)
        red_ref[...] = redbuf[3]

    _interleave([chunk(k) for k in range(CHUNKS)] + [w_proc(), red_proc(), dw_proc()])
    shared["o"].wait()
    for c in groups:
        c.wait_send()


def _finish(red_ref, dh_ref, dw_ref, loss_out, dh_out, dw_out, dg_out, redv, dhv, buf, lossv, dgv, sem):
    step = buf.shape[1] // 4
    cols = [(slice(None), pl.ds(i * step, step)) for i in range(4)]
    moves = [(red_ref, redv, None)] + [(dw_ref.at[c], buf.at[c], dw_out.at[c]) for c in cols] + [(dh_ref, dhv, dh_out)]
    gets = [pltpu.make_async_copy(a, b, sem.at[i, 0]) for i, (a, b, _) in enumerate(moves)]
    puts = [pltpu.make_async_copy(b, c, sem.at[i, 1]) for i, (_, b, c) in enumerate(moves) if c is not None]
    for g in gets:
        g.start()
    gets[0].wait()
    lossv[...] = redv[:, dgv.shape[1]:dgv.shape[1] + 1]
    dgv[...] = redv[:, :dgv.shape[1]]
    puts += [pltpu.make_async_copy(lossv, loss_out, sem.at[0, 1]), pltpu.make_async_copy(dgv, dg_out, sem.at[6, 1])]
    for p in puts[5:]:
        p.start()
    for g, p in zip(gets[1:], puts):
        g.wait()
        p.start()
    for p in puts:
        p.wait()


def solution(mesh):
    def local_step(hidden, labels, loss_weight, norm_gain, w_local):
        rows, depth = hidden.shape
        vloc = w_local.shape[1]
        vreal = vloc * mesh.shape["vp"] - PAD_COLS
        vm = pl.BlockSpec(memory_space=pltpu.VMEM)
        hbm = pl.BlockSpec(memory_space=pl.ANY)
        scratch = _scratch(rows, depth, vloc)
        red, dh, dwt = pl.pallas_call(
            functools.partial(_kernel, (rows, depth, vloc, vreal), tuple(scratch)),
            name="head_step",
            out_shape=(jax.ShapeDtypeStruct((1, depth + 256), F32),
                       jax.ShapeDtypeStruct((rows, depth), BF16),
                       jax.ShapeDtypeStruct((vloc, depth), F32)),
            in_specs=[hbm] * 5,
            out_specs=(vm, vm, hbm),
            scratch_shapes=list(scratch.values()),
            compiler_params=pltpu.CompilerParams(
                collective_id=0, has_side_effects=True, vmem_limit_bytes=63 * 1024 * 1024),
        )(labels.reshape(1, rows), loss_weight.reshape(1, rows), hidden, norm_gain.reshape(1, depth), w_local.T)
        loss, dh, dwt, dg = pl.pallas_call(
            _finish,
            name="head_out",
            out_shape=(jax.ShapeDtypeStruct((1, 1), F32),
                       jax.ShapeDtypeStruct((rows, depth), BF16),
                       jax.ShapeDtypeStruct((vloc, depth), F32),
                       jax.ShapeDtypeStruct((1, depth), F32)),
            in_specs=[hbm] * 3,
            out_specs=[hbm] * 4,
            scratch_shapes=[pltpu.VMEM((1, depth + 256), F32), pltpu.VMEM((rows, depth), BF16),
                            pltpu.VMEM((vloc, depth), F32), pltpu.VMEM((1, 1), F32), pltpu.VMEM((1, depth), F32),
                            pltpu.SemaphoreType.DMA((7, 2))],
        )(red, dh, dwt)
        return loss.reshape(1), dh, dwt.T, dg.reshape(depth)

    return jax.shard_map(
        local_step,
        mesh=mesh,
        in_specs=(P(("dp", "vp"), None), P(("dp", "vp")), P(("dp", "vp")), P(None), P(None, "vp")),
        out_specs=(P("dp"), P(("dp", "vp"), None), P("dp", "vp"), P("dp")),
        check_vma=False,
    )
```
